32 devices in a mesh: dp: 16 (over z, x, core), tensor: 2 (over y).
Axes of the slice: x: 2, y: 2, z: 4, core: 2. Of those that a mesh axis runs over, the one named last changes fastest.
Arguments:
- hidden_in: bfloat16 [8192, 2048], P('dp'), may hold values from -6 to 6
- segments: int32 [16, 512], P('dp'), may hold values from 0 to 3, never falling along the last dimension, each value on 1 to 256 neighbouring positions
- cotangent: bfloat16 [8192, 2048], P('dp'), may hold values from -6 to 6
- w_query: bfloat16 [2048, 2048], P('dp', 'tensor'), may hold values from -0.125 to 0.125
- w_key: bfloat16 [2048, 2048], P('dp', 'tensor'), may hold values from -0.125 to 0.125
- w_value: bfloat16 [2048, 2048], P('dp', 'tensor'), may hold values from -0.125 to 0.125
- w_dense: bfloat16 [2048, 2048], P('tensor', 'dp'), may hold values from -0.5 to 0.5
- w_up: bfloat16 [2048, 8192], P('dp', 'tensor'), may hold values from -0.125 to 0.125
- w_down: bfloat16 [8192, 2048], P('tensor', 'dp'), may hold values from -0.0625 to 0.0625
- bias_query: bfloat16 [8, 256], P('tensor', 'dp'), may hold values from -3 to 3
- bias_key: bfloat16 [8, 256], P('tensor', 'dp'), may hold values from -3 to 3
- bias_value: bfloat16 [8, 256], P('tensor', 'dp'), may hold values from -3 to 3
- bias_dense: bfloat16 [2048], P('dp'), may hold values from -3 to 3
- bias_up: bfloat16 [32, 256], P('tensor', 'dp'), may hold values from -3 to 3
- bias_down: bfloat16 [2048], P('dp'), may hold values from -3 to 3
- attend_gain: bfloat16 [2048], P('dp'), may hold values from 0.099609375 to 1.8984375
- attend_shift: bfloat16 [2048], P('dp'), may hold values from -2 to 2
- feed_gain: bfloat16 [2048], P('dp'), may hold values from 0.099609375 to 1.8984375
- feed_shift: bfloat16 [2048], P('dp'), may hold values from -2 to 2
Outputs:
- hidden_out: bfloat16 [8192, 2048], P('dp')
- grad_input: float32 [8192, 2048], P('dp')
- grad_w_query: float32 [2048, 2048], P('dp', 'tensor')
- grad_w_key: float32 [2048, 2048], P('dp', 'tensor')
- grad_w_value: float32 [2048, 2048], P('dp', 'tensor')
- grad_w_dense: float32 [2048, 2048], P('tensor', 'dp')
- grad_w_up: float32 [2048, 8192], P('dp', 'tensor')
- grad_w_down: float32 [8192, 2048], P('tensor', 'dp')
- grad_bias_query: float32 [8, 256], P('tensor', 'dp')
- grad_bias_key: float32 [8, 64], P('tensor')
- grad_bias_value: float32 [8, 256], P('tensor', 'dp')
- grad_bias_dense: float32 [2048], P('dp')
- grad_bias_up: float32 [32, 256], P('tensor', 'dp')
- grad_bias_down: float32 [2048], P('dp')
- grad_attend_gain: float32 [2048], P('dp')
- grad_attend_shift: float32 [2048], P('dp')
- grad_feed_gain: float32 [2048], P('dp')
- grad_feed_shift: float32 [2048], P('dp')
The draws below stay inside these ranges and needn't reach their ends.
Inputs may be any that keep to these rules, and one draw needn't show every extreme that they name: `segments`: within each packed row the segment numbers never fall; each segment holds 1 to 256 tokens and one holds exactly that many.
All inputs are finite; a program needn't handle non-finite values.
Results may differ from the reference program's by a relative error of at most 0.012.
The reference program's roundings to bfloat16 on the way count: a program that leaves them out, or rounds other values in their place, can miss the bound.
Values may be sent and summed in bfloat16 or wider, within the bound.
A program may use at most 256 MiB of HBM per device.

```python
import math
import jax
import jax.numpy as jnp
import numpy as np
from jax import lax

D = 2048
FF = 8192
HEADS = 8
HD = 256
ROT = 64
TOK_DEV = 512
SEQS = 16
TOKENS = 8192


def spiked(array, own_key, source, target, blocks, factor):
    def block_of(dim):
        return (jnp.arange(array.shape[dim]) // (array.shape[dim] // blocks)).reshape((-1,) + (1,) * (array.ndim - 1 - dim))

    one_side = jax.random.permutation(own_key, blocks)[block_of(target)]
    far = (block_of(target) + blocks // 2) % blocks
    return jnp.where((block_of(source) == one_side) | (block_of(source) == far), factor * array, array)


def shard_levels(own_key, extent, cuts, smallest, top_value):
    level = 1.0
    for position, parts in cuts:
        draws = jax.random.uniform(jax.random.fold_in(jax.random.fold_in(own_key, 6), position), (parts,), jnp.float32, smallest / len(cuts), top_value / len(cuts))
        level = level * jnp.repeat(jnp.exp(draws), extent[position] // parts).reshape((-1,) + (1,) * (len(extent) - 1 - position))
    return level


def profile(number_of, total, reach, skew):
    portions = [(1 << 20) // math.isqrt(standing ** skew) + 1 for standing in range(2, number_of + 1)]
    surplus, counts = total - reach - (number_of - 1), [1] * (number_of - 1)
    while surplus > 0:
        free = [i for i in range(number_of - 1) if counts[i] < reach]
        mass, budget = sum([portions[i] for i in free]), surplus
        for i in free:
            extra = min(reach - counts[i], max(1, budget * portions[i] // mass), surplus)
            counts[i] = counts[i] + extra
            surplus = surplus - extra
    return np.array([reach] + counts)


def uneven(rng, number_of, total, reach, lean):
    if number_of == 2:
        one = jax.random.randint(rng, (), max(1, total - reach), min(reach, total - 1) + 1)
        return jnp.stack([one, total - one])
    lengths = jnp.asarray(profile(number_of, total, reach, lean), jnp.int32)
    pairs = (number_of - 1) // 2
    source_of, receiver = lengths[1:1 + 2 * pairs:2], lengths[2:2 + 2 * pairs:2]
    room = jnp.minimum(source_of - 1, reach - receiver)
    moved = jax.random.randint(jax.random.fold_in(rng, 1), (pairs,), 0, 1 << 20) % (room + 1)
    lengths = lengths.at[1:1 + 2 * pairs:2].set(source_of - moved).at[2:2 + 2 * pairs:2].set(receiver + moved)
    return lengths[jax.random.permutation(jax.random.fold_in(rng, 2), number_of)]


def scatter_about(key, shape, scale, reach, pieces=(), kind=jnp.bfloat16):
    array = jax.random.normal(key, shape, jnp.float32) * scale
    if len(pieces) > 0:
        array = shard_levels(key, shape, pieces, -0.22, 0.18) * array
    return jnp.clip(array, min=-reach, max=reach).astype(kind)


def noise_with(own_key, dims, scale, limit, pieces, heavy, kind=jnp.bfloat16):
    entries = scale * jax.random.normal(own_key, dims, jnp.float32)
    if pieces:
        entries = entries * shard_levels(own_key, dims, pieces, -0.22, 0.18)
    return jnp.clip(spiked(entries, jax.random.fold_in(own_key, 3), *heavy), -limit, limit).astype(kind)


def setup_inputs(seed: int = 0) -> dict:
    seeds = jax.random.split(jax.random.key(seed), 20)
    return {
        "hidden_in": noise_with(seeds[0], (TOKENS, D), 1.0, 6.0, ((0, 16),), (0, 1, 16, 2.0)),
        "segments": jax.vmap(lambda own: jnp.searchsorted(jnp.cumsum(uneven(own, 4, TOK_DEV, TOK_DEV // 2, 1)), jnp.arange(TOK_DEV), side="right"))(jax.random.split(seeds[1], SEQS)).reshape((SEQS, TOK_DEV)).astype(jnp.int32),
        "cotangent": noise_with(seeds[2], (TOKENS, D), 1.0, 6.0, ((0, 16),), (0, 1, 16, 2.0)),
        "w_query": scatter_about(seeds[3], (D, D), D ** -0.5, 0.125, ((0, 16), (1, 2))),
        "w_key": scatter_about(seeds[4], (D, D), D ** -0.5, 0.125, ((0, 16), (1, 2))),
        "w_value": scatter_about(seeds[5], (D, D), D ** -0.5, 0.125, ((0, 16), (1, 2))),
        "w_dense": scatter_about(seeds[6], (D, D), (D // 16) ** -0.5, 0.5, ((0, 2), (1, 16))),
        "w_up": scatter_about(seeds[7], (D, FF), D ** -0.5, 0.125, ((0, 16), (1, 2))),
        "w_down": scatter_about(seeds[8], (FF, D), FF ** -0.5, 0.0625, ((0, 2), (1, 16))),
        "bias_query": scatter_about(seeds[9], (HEADS, HD), 0.5, 3.0, ((0, 2), (1, 16))),
        "bias_key": scatter_about(seeds[10], (HEADS, HD), 0.5, 3.0, ((0, 2), (1, 16))),
        "bias_value": scatter_about(seeds[11], (HEADS, HD), 0.5, 3.0, ((0, 2), (1, 16))),
        "bias_dense": scatter_about(seeds[12], (D,), 0.5, 3.0, ((0, 16),)),
        "bias_up": scatter_about(seeds[13], (FF // HD, HD), 0.5, 3.0, ((0, 2), (1, 16))),
        "bias_down": scatter_about(seeds[14], (D,), 0.5, 3.0, ((0, 16),)),
        "attend_gain": jnp.clip(1.0 + 0.18 * jax.random.normal(seeds[15], (D,), jnp.float32), 0.099609375, 1.8984375).astype(jnp.bfloat16),
        "attend_shift": scatter_about(seeds[16], (D,), 0.3, 2.0, ((0, 16),)),
        "feed_gain": jnp.clip(1.0 + 0.18 * jax.random.normal(seeds[17], (D,), jnp.float32), 0.099609375, 1.8984375).astype(jnp.bfloat16),
        "feed_shift": scatter_about(seeds[18], (D,), 0.3, 2.0, ((0, 16),)),
    }


@jax.custom_vjp
def low(v):
    return lax.optimization_barrier(v.astype(jnp.bfloat16)).astype(jnp.float32)

@jax.custom_vjp
def low_back(v):
    return v

def low_keep(v):
    return (low(v), None)

def low_pass(kept, grad):
    return (grad,)

def back_keep(v):
    return (v, None)

def back_low(kept, grad):
    return (low(grad),)
low.defvjp(low_keep, low_pass)
low_back.defvjp(back_keep, back_low)

def layer_norm(tokens, gain_vec, shift_vec):
    average = lax.optimization_barrier(jnp.mean(tokens, axis=-1, keepdims=True))
    centred = tokens - average
    spread = lax.optimization_barrier(jnp.mean(centred * centred, axis=-1, keepdims=True))
    return centred * lax.rsqrt(spread + 1e-05) * gain_vec + shift_vec

def row_layout(segment_row):
    places = jnp.arange(TOK_DEV, dtype=jnp.int32)
    same_doc = segment_row[:, None] == segment_row[None, :]
    starts = lax.optimization_barrier(jnp.min(jnp.where(same_doc, places[None, :], TOK_DEV), axis=1)).astype(jnp.int32)
    allowed = same_doc & (places[None, :] <= places[:, None])
    return (allowed, places - starts)

def rotary_tables(positions):
    steps_in = jnp.arange(ROT // 2).astype(jnp.float32)
    inverse_freq = 10000.0 ** (-2.0 * steps_in / ROT)
    angles = positions.astype(jnp.float32)[:, None] * inverse_freq[None, :]
    return (jnp.cos(angles)[:, None, :], jnp.sin(angles)[:, None, :])

def rotate(states, cosine, sine_table):
    halfway = ROT // 2
    front_part = states[..., :halfway]
    back_part = states[..., halfway:ROT]
    return jnp.concatenate([front_part * cosine - back_part * sine_table, back_part * cosine + front_part * sine_table, states[..., ROT:]], axis=-1)

def attend_row(operands):
    query_row, key_row, value_row, segment_row = operands
    allowed, positions = row_layout(segment_row)
    cosine, sine_table = rotary_tables(positions)
    query_rot = low(rotate(query_row, cosine, sine_table))
    key_rot = low(rotate(key_row, cosine, sine_table))
    value_low = low(value_row)
    scores = jnp.einsum('qhd,khd->hqk', query_rot, key_rot, precision=lax.Precision.HIGHEST) * HD ** (-0.5)
    scores = low_back(scores)
    scores = jnp.where(allowed[None], scores, -1e+30)
    row_top = lax.optimization_barrier(jnp.max(scores, axis=-1, keepdims=True))
    exp_scores = jnp.exp(scores - row_top)
    probs_full = low(exp_scores / lax.optimization_barrier(jnp.sum(exp_scores, axis=-1, keepdims=True)))
    return jnp.einsum('hqk,khd->qhd', probs_full, value_low, precision=lax.Precision.HIGHEST)

def matmul(left, right):
    return jnp.dot(left, right, precision=lax.Precision.HIGHEST)

def group_forward(params, tokens, segment_rows):
    w_query, w_key, w_value, w_dense, w_up, w_down, bias_query, bias_key, bias_value, bias_dense, bias_up, bias_down, attend_gain, attend_shift, feed_gain, feed_shift = params
    row_count = segment_rows.shape[0]
    normed_attend = low(layer_norm(tokens, attend_gain, attend_shift))
    normed_feed = low(layer_norm(tokens, feed_gain, feed_shift))
    query_lin = low_back(matmul(normed_attend, w_query) + bias_query.reshape(-1))
    key_lin = low_back(matmul(normed_attend, w_key) + bias_key.reshape(-1))
    value_lin = low_back(matmul(normed_attend, w_value) + bias_value.reshape(-1))
    shaped = (row_count, TOK_DEV, HEADS, HD)
    attended = lax.map(jax.checkpoint(attend_row), (query_lin.reshape(shaped), key_lin.reshape(shaped), value_lin.reshape(shaped), segment_rows))
    attended = low(low_back(attended.reshape(row_count * TOK_DEV, D)))
    attention_out = matmul(attended, w_dense)
    pre_act = low_back(matmul(normed_feed, w_up) + bias_up.reshape(-1))
    activated = low(jax.nn.gelu(pre_act, approximate=False))
    feed_out = matmul(activated, w_down)
    return tokens + attention_out + feed_out + bias_dense + bias_down

def reference(hidden_in, segments, cotangent, w_query, w_key, w_value, w_dense, w_up, w_down, bias_query, bias_key, bias_value, bias_dense, bias_up, bias_down, attend_gain, attend_shift, feed_gain, feed_shift):
    params = tuple((arr.astype(jnp.float32) for arr in (w_query, w_key, w_value, w_dense, w_up, w_down, bias_query, bias_key, bias_value, bias_dense, bias_up, bias_down, attend_gain, attend_shift, feed_gain, feed_shift)))
    rows_per = math.gcd(SEQS, max(1, 4096 // TOK_DEV))
    groups = SEQS // rows_per
    tokens_all = hidden_in.astype(jnp.float32).reshape(groups, rows_per * TOK_DEV, D)
    cot_all = cotangent.astype(jnp.float32).reshape(groups, rows_per * TOK_DEV, D)
    segment_all = segments.reshape(groups, rows_per, TOK_DEV)

    def scan_step(totals, inputs):
        tokens, segment_rows, cot_rows = inputs

        def inner(weights_in, tok_rows):
            return group_forward(weights_in, tok_rows, segment_rows)
        output, pullback = jax.vjp(inner, params, tokens)
        grads_params, grads_tokens = pullback(cot_rows)
        totals = jax.tree.map(jnp.add, totals, grads_params)
        return (totals, (output, grads_tokens))
    zeros_init = jax.tree.map(jnp.zeros_like, params)
    totals, (outputs, grads_tokens) = lax.scan(scan_step, zeros_init, (tokens_all, segment_all, cot_all))
    hidden_out = outputs.reshape(TOKENS, D).astype(jnp.bfloat16)
    grad_input = grads_tokens.reshape(TOKENS, D)
    return (hidden_out, grad_input, totals[0], totals[1], totals[2], totals[3], totals[4], totals[5], totals[6], totals[7][:, :ROT], totals[8], totals[9], totals[10], totals[11], totals[12], totals[13], totals[14], totals[15])
```

```python
import functools

import jax
import jax.numpy as jnp
from jax import lax
from jax.experimental import pallas as pl
from jax.experimental.pallas import tpu as pltpu
from jax.sharding import PartitionSpec as P

HD = 256
ROT = 64
TP = 4
LANES = 128
BC = 2 * HD
BF = jnp.bfloat16
F32 = jnp.float32
MESH = pl.DeviceIdType.MESH
OWN_SLOTS = 4
W_SLOTS = 3


def dot_nn(a, b):
    return lax.dot_general(a, b, (((1,), (0,)), ((), ())), preferred_element_type=F32)


def dot_nt(a, b):
    return lax.dot_general(a, b, (((1,), (1,)), ((), ())), preferred_element_type=F32)


def dot_tn(a, b):
    return lax.dot_general(a, b, (((0,), (0,)), ((), ())), preferred_element_type=F32)


def normed_hat(x):
    mean = jnp.mean(x, axis=-1, keepdims=True)
    centred = x - mean
    inverse = lax.rsqrt(jnp.mean(centred * centred, axis=-1, keepdims=True) + 1e-05)
    return centred * inverse, inverse


def swap_halves(u):
    half = ROT // 2
    lane = lax.broadcasted_iota(jnp.int32, u.shape, 1)
    return jnp.where(lane < half, pltpu.roll(u, LANES - half, 1), pltpu.roll(u, half, 1))


def turn(u, cosine, sine):
    head = u[:, :LANES]
    return jnp.concatenate([head * cosine + swap_halves(head) * sine, u[:, LANES:]], axis=1)


def attend(normed, cot, w_qk, w_vd, bias, table):
    scale = HD ** (-0.5)
    tokens = normed.shape[0]
    q = dot_nn(normed, w_qk[:, :HD]) + bias[:, :HD]
    k = dot_nn(normed, w_qk[:, HD:]) + bias[:, HD : 2 * HD]
    v = dot_nn(normed, w_vd[:, :HD]) + bias[:, 2 * HD :]
    grad_att = dot_nn(cot, w_vd[:, HD:]).astype(BF)
    half = ROT // 2
    lane = lax.broadcasted_iota(jnp.int32, table.shape, 1)
    later, sooner = pltpu.roll(table, half, 1), pltpu.roll(table, LANES - half, 1)
    cosine = jnp.where(lane < half, table, jnp.where(lane < ROT, later, 1.0))
    sine = jnp.where(lane < half, -sooner, jnp.where(lane < ROT, table, 0.0))
    start = table[:, ROT : ROT + 1]
    q_rot = turn(q, cosine, sine).astype(BF)
    k_rot = turn(k, cosine, sine).astype(BF)
    v_low = v.astype(BF)
    scores = dot_nt(q_rot, k_rot) * scale
    row = lax.broadcasted_iota(jnp.int32, (tokens, tokens), 0)
    col = lax.broadcasted_iota(jnp.int32, (tokens, tokens), 1)
    allowed = (col <= row) & (col >= start.astype(jnp.int32))
    scores = jnp.where(allowed, scores, -1e30)
    top = jnp.max(scores, axis=-1, keepdims=True)
    weights = jnp.exp(scores - top)
    probs = weights / jnp.sum(weights, axis=-1, keepdims=True)
    probs_low = probs.astype(BF)
    attended = dot_nn(probs_low, v_low).astype(BF)
    grad_probs = dot_nt(grad_att, v_low)
    delta = jnp.sum(probs * grad_probs, axis=-1, keepdims=True)
    grad_scores = (probs * (grad_probs - delta)).astype(BF)
    grad_q = turn(dot_nn(grad_scores, k_rot) * scale, cosine, -sine).astype(BF)
    grad_k = turn(dot_tn(grad_scores, q_rot) * scale, cosine, -sine).astype(BF)
    grad_v = dot_tn(probs_low, grad_att).astype(BF)
    return grad_q, grad_k, grad_v, attended


def main_kernel(cfg, *refs):
    groups, part, depth, width, tokens, length, feeds, back = cfg
    blocks = feeds + 2
    feed_of = {b: i for i, b in enumerate([0, 1] + list(range(4, blocks)))}
    (
        x_in,
        cot_in,
        w_query,
        w_key,
        w_value,
        dense_t,
        w_up,
        down_t,
        norms,
        bias,
        table,
        x_all,
        w_all,
        ga_out,
        act_out,
        pre_out,
        bk_out,
        sums_out,
        from_left,
        from_right,
        big,
        wv,
        own,
        fin,
        ld,
        xs,
        act_v,
        ga_v,
        a2a_s,
        a2a_r,
        tok_s,
        tok_r,
        ag_s,
        ag_r,
        rs_s,
        rs_r,
        bk_s,
        bk_r,
        loc,
    ) = refs
    dp, ty = lax.axis_index("dp"), lax.axis_index("tensor")
    rank, z = lax.rem(dp, TP), lax.div(dp, TP)
    hidden = w_up.shape[1] // TP

    def remote(src, dst, ssem, rsem, target):
        return pltpu.make_async_remote_copy(
            src_ref=src,
            dst_ref=dst,
            send_sem=ssem,
            recv_sem=rsem,
            device_id=(target, ty),
            device_id_type=MESH,
        )

    peer = [dp] + [lax.bitwise_xor(dp, k) for k in range(1, TP)]
    prank = [rank] + [lax.bitwise_xor(rank, k) for k in range(1, TP)]
    step_of = (TP, -TP)

    def local(src, dst, sem):
        return pltpu.make_async_copy(src, dst, sem)

    def sources(b):
        if b == 2:
            return ((w_query, HD, 0), (w_key, HD, 0))
        if b == 3:
            return ((w_value, HD, 0), (dense_t, HD, 0))
        i = feed_of[b]
        return ((w_up, hidden, i * HD), (down_t, hidden, i * HD))

    def a2a_copy(b, k, half, receiving):
        array, size, offset = sources(b)[half]
        cols = pl.ds(pl.multiple_of(prank[k] * size + offset, LANES), HD)
        owner = prank[k] if receiving else rank
        rows = pl.ds(pl.multiple_of(z * part + owner * depth, depth), depth)
        dst = w_all.at[b, rows, pl.ds(half * HD, HD)]
        if k == 0:
            return local(array.at[:, cols], dst, a2a_r.at[b, k, half])
        return remote(
            array.at[:, cols], dst, a2a_s.at[b, k, half], a2a_r.at[b, k, half], peer[k]
        )

    def a2a_start(b):
        for k in (2, 3, 1, 0):
            for half in range(2):
                a2a_copy(b, k, half, False).start()

    def a2a_wait(b):
        for k in range(TP):
            for half in range(2):
                copy = a2a_copy(b, k, half, True)
                if k == 0:
                    copy.wait()
                else:
                    copy.wait_recv()

    def tok_copy(which, hop):
        ssem, rsem = tok_s.at[which, hop], tok_r.at[which, hop]
        if which == 0:
            src, at = x_in, lambda k: x_all.at[k]
        else:
            src, at = cot_in, lambda k: big.at[2, pl.ds(k * length, length), :]
        if hop == 0:
            return local(src, at(0), rsem)
        if hop == 1:
            return remote(src, at(1), ssem, rsem, peer[1])
        if hop == 2:
            return remote(src, at(2), ssem, rsem, peer[2])
        return remote(at(2), at(3), ssem, rsem, peer[1])

    def tok_start(which):
        for hop in (2, 1, 0):
            tok_copy(which, hop).start()

    def tok_forward(which):
        tok_copy(which, 2).wait_recv()
        tok_copy(which, 3).start()

    def norm_slot(k):
        src = x_in if k == 0 else x_all.at[k]
        copy = local(src, xs, loc.at[0])
        copy.start()
        copy.wait()
        rows = min(64, length)

        def body(i, carry):
            at = pl.ds(pl.multiple_of(i * rows, rows), rows)
            hat, _ = normed_hat(xs[at, :].astype(F32))
            to = pl.ds(pl.multiple_of(k * length + i * rows, rows), rows)
            big[0, to, :] = (hat * norms[0:1, :] + norms[1:2, :]).astype(BF)
            big[1, to, :] = (hat * norms[2:3, :] + norms[3:4, :]).astype(BF)
            return carry

        lax.fori_loop(0, length // rows, body, 0)

    def ag_copy(b, s, way, g):
        at = w_all.at[b, pl.ds(pl.multiple_of(g * part, part), part), :]
        return remote(
            at, at, ag_s.at[b, s, way], ag_r.at[b, s, way], lax.rem(dp + step_of[way] + dp_size, dp_size)
        )

    dp_size = groups * TP

    def ag_step(b, s):
        @pl.when((z >= s - 1) & (z <= groups - 2))
        def _():
            g = z - s + 1
            if s > 1:
                ag_copy(b, s - 1, 0, g).wait_recv()
            ag_copy(b, s, 0, g).start()

        @pl.when((z <= groups - s) & (z >= 1))
        def _():
            g = z + s - 1
            if s > 1:
                ag_copy(b, s - 1, 1, g).wait_recv()
            ag_copy(b, s, 1, g).start()

    def ag_finish(b):
        @pl.when(z == groups - 1)
        def _():
            for s in range(1, groups):
                ag_copy(b, s, 0, z - s).wait_recv()

        @pl.when(z == 0)
        def _():
            for s in range(1, groups):
                ag_copy(b, s, 1, z + s).wait_recv()

    def ag_drain(b):
        for s in range(1, groups):

            @pl.when((z >= s - 1) & (z <= groups - 2))
            def _():
                ag_copy(b, s, 0, z - s + 1).wait_send()

            @pl.when((z <= groups - s) & (z >= 1))
            def _():
                ag_copy(b, s, 1, z + s - 1).wait_send()

    def rs_copy(b, t, way, d):
        land = (from_left, from_right)[way]
        return remote(
            own.at[b % OWN_SLOTS, d],
            land.at[b, t - 1],
            rs_s.at[b, t, way],
            rs_r.at[b, t, way],
            lax.rem(dp + step_of[way] + dp_size, dp_size),
        )

    rows_add = min(64, BC)

    def load(b, t, way):
        return local((from_left, from_right)[way].at[b, t - 1], ld.at[way], loc.at[1 + way])

    def add_in(b, d, way):
        slot = b % OWN_SLOTS

        def body(i, carry):
            at = pl.ds(pl.multiple_of(i * rows_add, rows_add), rows_add)
            own[slot, d, at, :] = (own[slot, d, at, :].astype(F32) + ld[way, at, :].astype(F32)).astype(BF)
            return carry

        lax.fori_loop(0, BC // rows_add, body, 0)

    def rs_conditions(t):
        return (z <= t - 1, z >= groups - t)

    def rs_step(b, t):
        go = rs_conditions(t)
        ends = (z == 0, z == groups - 1)
        dest = (z + groups - t, z - groups + t)
        for way in range(2):
            d = dest[way]
            if t > 1:

                @pl.when(go[way] & jnp.logical_not(ends[way]))
                def _():
                    rs_copy(b, t - 1, way, d).wait_recv()
                    load(b, t - 1, way).start()

        for way in range(2):
            d = dest[way]
            if t > 1:

                @pl.when(go[way] & jnp.logical_not(ends[way]))
                def _():
                    load(b, t - 1, way).wait()
                    add_in(b, d, way)

            @pl.when(go[way])
            def _():
                rs_copy(b, t, way, d).start()

    def rs_drain(b):
        for t in range(1, groups):
            go = rs_conditions(t)

            @pl.when(go[0])
            def _():
                rs_copy(b, t, 0, z + groups - t).wait_send()

            @pl.when(go[1])
            def _():
                rs_copy(b, t, 1, z - groups + t).wait_send()

    def bk_copy(b, k, receiving=False):
        src = fin.at[b % 2]
        if back != part:
            src = src.at[:, pl.ds(pl.multiple_of(prank[k] * depth, LANES), depth)]
        dst = bk_out.at[k, b]
        if k == 0:
            return local(src, dst, bk_r.at[b, k])
        return remote(src, dst, bk_s.at[b, k], bk_r.at[b, k], peer[k])

    def bk_drain(b):
        bk_copy(b, 0).wait()
        for k in range(1, TP):
            bk_copy(b, k).wait_send()

    def rs_finish(b):
        last = groups - 1
        inner = (z > 0, z < groups - 1)
        for way in range(2):

            @pl.when(inner[way])
            def _():
                rs_copy(b, last, way, z).wait_recv()
                load(b, last, way).start()

        if b >= 2:
            bk_drain(b - 2)
        for way in range(2):

            @pl.when(inner[way])
            def _():
                load(b, last, way).wait()

        slot = b % OWN_SLOTS

        def close(ways):
            def body(i, carry):
                at = pl.ds(pl.multiple_of(i * rows_add, rows_add), rows_add)
                total = own[slot, z, at, :].astype(F32)
                for way in ways:
                    total += ld[way, at, :].astype(F32)
                fin[b % 2, at, :] = total.astype(BF)
                return carry

            lax.fori_loop(0, BC // rows_add, body, 0)

        pl.when(z == 0)(lambda: close((1,)))
        pl.when(z == groups - 1)(lambda: close((0,)))
        pl.when((z > 0) & (z < groups - 1))(lambda: close((0, 1)))
        for k in (2, 3, 1, 0):
            bk_copy(b, k).start()

    def w_load(b, slot):
        return local(w_all.at[b], wv.at[slot], loc.at[3 + slot])

    def act_store(b, which):
        dst = (act_out, pre_out)[which].at[feed_of[b]]
        return local(act_v.at[which], dst, loc.at[3 + W_SLOTS + which])

    def feed_forward(b, slot):
        i = feed_of[b]
        first = i * HD

        def body(n, carry):
            at = pl.ds(pl.multiple_of(n * length, length), length)
            pre = dot_nn(big[1, at, :], wv[slot, :, :HD]) + bias[:, 3 * HD + first : 4 * HD + first]
            grad_act = dot_nn(big[2, at, :], wv[slot, :, HD:])
            cdf = 0.5 * (1.0 + lax.erf(pre * 0.7071067811865476))
            pdf = jnp.exp(-0.5 * pre * pre) * 0.3989422804014327
            act_v[0, at, :] = (pre * cdf).astype(BF)
            grad_pre = (grad_act * (cdf + pre * pdf)).astype(BF)
            act_v[1, at, :] = grad_pre
            return carry + jnp.sum(grad_pre.astype(F32), axis=0, keepdims=True)

        total = lax.fori_loop(0, TP, body, jnp.zeros((1, HD), F32))
        sums_out[0:1, 3 * HD + first : 4 * HD + first] = total

    def feed_backward(b):
        slot = b % OWN_SLOTS

        def body(d, carry):
            cols = pl.ds(pl.multiple_of(d * part, part), part)
            own[slot, d, :HD, :] = dot_tn(act_v[1], big[1, :, cols]).astype(BF)
            own[slot, d, HD:, :] = dot_tn(act_v[0], big[2, :, cols]).astype(BF)
            return carry

        lax.fori_loop(0, groups, body, 0)
        for which in range(2):
            act_store(b, which).start()

    def feed_stored(b):
        for which in range(2):
            act_store(b, which).wait()

    def attention(slot_qk, slot_vd, between):
        def body(n, carry):
            at = pl.ds(pl.multiple_of(n * length, length), length)
            grads = attend(
                big[0, at, :],
                big[2, at, :],
                wv.at[slot_qk],
                wv.at[slot_vd],
                bias[:, : 3 * HD],
                table[at, :],
            )
            for j, g in enumerate(grads):
                ga_v[at, j * HD : (j + 1) * HD] = g
            for j, events in enumerate(between):

                @pl.when(n == j)
                def _():
                    events()

            sums = [jnp.sum(g.astype(F32), axis=0, keepdims=True) for g in grads[:3]]
            return carry + jnp.concatenate(sums, axis=1)

        sums_out[0:1, : 3 * HD] = lax.fori_loop(0, TP, body, jnp.zeros((1, 3 * HD), F32))

    def attention_back(b):
        slot = b % OWN_SLOTS

        def body(d, carry):
            cols = pl.ds(pl.multiple_of(d * part, part), part)
            if b == 2:
                own[slot, d, :, :] = dot_tn(ga_v[:, :BC], big[0, :, cols]).astype(BF)
            else:
                own[slot, d, :HD, :] = dot_tn(ga_v[:, BC : 3 * HD], big[0, :, cols]).astype(BF)
                own[slot, d, HD:, :] = dot_tn(ga_v[:, 3 * HD :], big[2, :, cols]).astype(BF)
            return carry

        lax.fori_loop(0, groups, body, 0)

    barrier = pltpu.get_barrier_semaphore()
    for k in range(1, TP):
        pl.semaphore_signal(barrier, inc=1, device_id=(peer[k], ty), device_id_type=MESH)

    @pl.when(z > 0)
    def _():
        pl.semaphore_signal(barrier, inc=1, device_id=(dp - TP, ty), device_id_type=MESH)

    @pl.when(z < groups - 1)
    def _():
        pl.semaphore_signal(barrier, inc=1, device_id=(dp + TP, ty), device_id_type=MESH)

    inside = (z > 0) & (z < groups - 1)
    pl.when(inside)(lambda: pl.semaphore_wait(barrier, TP + 1))
    pl.when(jnp.logical_not(inside))(lambda: pl.semaphore_wait(barrier, TP))

    def ag_steps(b):
        for s in range(1, groups):
            ag_step(b, s)

    def rs_steps(b):
        for t in range(1, groups):
            rs_step(b, t)

    mid = max(1, groups - 2)

    def ag_part(b, first, last):
        for s in range(first, last + 1):
            ag_step(b, s)

    def rs_part(b, first, last):
        for t in range(first, last + 1):
            rs_step(b, t)

    def start_ag(b):
        a2a_wait(b)
        ag_step(b, 1)

    end = groups - 1
    a2a_start(0)
    tok_start(0)
    a2a_start(1)
    a2a_start(2)
    tok_start(1)
    for b in range(3, blocks):
        a2a_start(b)
    sums_out[...] = jnp.zeros(sums_out.shape, F32)
    norm_slot(0)
    start_ag(0)
    tok_copy(0, 1).wait_recv()
    norm_slot(1)
    ag_part(0, 2, end)
    tok_forward(0)
    start_ag(1)
    norm_slot(2)
    tok_copy(0, 3).wait_recv()
    norm_slot(3)
    ag_part(1, 2, end)
    start_ag(2)
    ag_part(2, 2, mid)
    tok_forward(1)
    ag_part(2, mid + 1, end)
    tok_copy(1, 0).wait()
    tok_copy(1, 1).wait_recv()
    ag_finish(0)
    w_load(0, 0).start()
    start_ag(3)
    ag_finish(1)
    w_load(1, 1).start()
    tok_copy(1, 3).wait_recv()
    w_load(0, 0).wait()
    feed_forward(0, 0)
    ag_part(3, 2, mid)
    feed_backward(0)
    rs_step(0, 1)
    ag_finish(2)
    w_load(2, 2).start()
    ag_part(3, mid + 1, end)
    rs_part(0, 2, mid)
    w_load(1, 1).wait()
    feed_stored(0)
    feed_forward(1, 1)
    start_ag(4)
    rs_part(0, mid + 1, end)
    feed_backward(1)
    rs_finish(0)
    rs_step(1, 1)
    ag_part(4, 2, mid)
    ag_finish(3)
    w_load(3, 0).start()
    w_load(2, 2).wait()
    w_load(3, 0).wait()
    feed_stored(1)

    def between0():
        rs_part(1, 2, mid)
        ag_part(4, mid + 1, end)

    def between1():
        start_ag(5)
        rs_part(1, mid + 1, end)

    def between2():
        ag_part(5, 2, mid)

    def between3():
        ag_part(5, mid + 1, end)

    attention(2, 0, [between0, between1, between2, between3])
    attention_back(2)
    rs_step(2, 1)
    rs_finish(1)
    attention_back(3)
    rs_part(2, 2, mid)
    ga_copy = local(ga_v, ga_out, loc.at[0])
    ga_copy.start()
    ag_finish(4)
    w_load(4, 1).start()
    ag_finish(5)
    w_load(5, 2).start()
    rs_part(2, mid + 1, end)
    rs_drain(0)
    w_load(4, 1).wait()
    feed_forward(4, 1)
    rs_step(3, 1)
    rs_finish(2)
    feed_backward(4)
    rs_part(3, 2, end)
    w_load(5, 2).wait()
    feed_stored(4)
    rs_drain(1)
    feed_forward(5, 2)
    rs_finish(3)
    rs_step(4, 1)
    feed_backward(5)
    rs_part(4, 2, end)
    rs_finish(4)
    rs_steps(5)
    rs_finish(5)
    feed_stored(5)
    ga_copy.wait()
    for b in range(blocks):
        for k in range(1, TP):
            for half in range(2):
                a2a_copy(b, k, half, False).wait_send()
        ag_drain(b)
        if b >= 2:
            rs_drain(b)
    tok_copy(0, 0).wait()
    for which in range(2):
        for hop in (1, 2, 3):
            tok_copy(which, hop).wait_send()
    bk_drain(blocks - 2)
    bk_drain(blocks - 1)
    for b in range(blocks):
        for k in range(1, TP):
            bk_copy(b, k).wait_recv()


def run_main(groups, x, cot, weights, norms, bias, table):
    length, width = x.shape
    depth = weights[0].shape[0]
    part = width // groups
    tokens = TP * length
    feeds = weights[4].shape[1] // TP // HD
    blocks = feeds + 2
    back = depth if depth % LANES == 0 else part
    cfg = (groups, part, depth, width, tokens, length, feeds, back)
    hbm = pl.BlockSpec(memory_space=pltpu.HBM)
    vmem = pl.BlockSpec(memory_space=pltpu.VMEM)
    sem = pltpu.SemaphoreType.DMA
    shape = jax.ShapeDtypeStruct
    return pl.pallas_call(
        functools.partial(main_kernel, cfg),
        out_shape=(
            shape((TP, length, width), BF),
            shape((blocks, width, BC), BF),
            shape((tokens, 4 * HD), BF),
            shape((feeds, tokens, HD), BF),
            shape((feeds, tokens, HD), BF),
            shape((TP, blocks, BC, back), BF),
            shape((8, bias.shape[1]), F32),
            shape((blocks, groups, BC, part), BF),
            shape((blocks, groups, BC, part), BF),
        ),
        in_specs=[hbm] * 8 + [vmem] * 3,
        out_specs=(hbm,) * 6 + (vmem,) + (hbm,) * 2,
        scratch_shapes=[
            pltpu.VMEM((3, tokens, width), BF),
            pltpu.VMEM((W_SLOTS, width, BC), BF),
            pltpu.VMEM((OWN_SLOTS, groups, BC, part), BF),
            pltpu.VMEM((2, BC, part), BF),
            pltpu.VMEM((2, BC, part), BF),
            pltpu.VMEM((length, width), BF),
            pltpu.VMEM((2, tokens, HD), BF),
            pltpu.VMEM((tokens, 4 * HD), BF),
            sem((blocks, TP, 2)),
            sem((blocks, TP, 2)),
            sem((2, 4)),
            sem((2, 4)),
            sem((blocks, groups, 2)),
            sem((blocks, groups, 2)),
            sem((blocks, groups, 2)),
            sem((blocks, groups, 2)),
            sem((blocks, TP)),
            sem((blocks, TP)),
            sem((3 + W_SLOTS + 2,)),
        ],
        compiler_params=pltpu.CompilerParams(
            collective_id=0, has_side_effects=True, vmem_limit_bytes=63 << 20
        ),
        name="main",
    )(x, cot, *weights, norms, bias, table)


def out_kernel(ga, act, w, out):
    feeds = act.shape[0]
    order = [0, 1] + list(range(4, feeds + 2))
    total = dot_nt(ga[:, 3 * HD :], w[3, :, HD:])
    for i, b in enumerate(order):
        total += dot_nt(act[i], w[b, :, HD:])
    out[...] = total.astype(BF)


def close_out(ga, act, w, rows):
    tokens, width = ga.shape[0], w.shape[1]
    feeds = act.shape[0]
    return pl.pallas_call(
        out_kernel,
        grid=(tokens // rows,),
        out_shape=jax.ShapeDtypeStruct((tokens, width), BF),
        in_specs=[
            pl.BlockSpec((rows, ga.shape[1]), lambda i: (i, 0)),
            pl.BlockSpec((feeds, rows, HD), lambda i: (0, i, 0)),
            pl.BlockSpec(w.shape, lambda i: (0, 0, 0)),
        ],
        out_specs=pl.BlockSpec((rows, width), lambda i: (i, 0)),
        compiler_params=pltpu.CompilerParams(vmem_limit_bytes=56 << 20),
        name="close_out",
    )(ga, act, w)


def back_kernel(x, gains, ga, pre, w, out, sums_out):
    feeds = pre.shape[0]
    order = [0, 1] + list(range(4, feeds + 2))
    hat, _ = normed_hat(x[...].astype(F32))
    grad_a = dot_nt(ga[:, :BC], w[2]) + dot_nt(ga[:, BC : 3 * HD], w[3, :, :HD])
    grad_f = dot_nt(pre[0], w[0, :, :HD])
    for i, b in enumerate(order[1:]):
        grad_f += dot_nt(pre[i + 1], w[b, :, :HD])
    out[...] = (grad_a * gains[0:1, :] + grad_f * gains[1:2, :]).astype(BF)
    col = lambda v: jnp.sum(v, axis=0, keepdims=True)
    zero = jnp.zeros((4, x.shape[1]), F32)
    sums = jnp.concatenate(
        [col(grad_a * hat), col(grad_a), col(grad_f * hat), col(grad_f), zero], axis=0
    )

    @pl.when(pl.program_id(0) == 0)
    def _():
        sums_out[...] = sums

    @pl.when(pl.program_id(0) > 0)
    def _():
        sums_out[...] += sums


def close_back(x, gains, ga, pre, w, rows):
    tokens, width = x.shape
    feeds = pre.shape[0]
    return pl.pallas_call(
        back_kernel,
        grid=(tokens // rows,),
        out_shape=(
            jax.ShapeDtypeStruct((tokens, width), BF),
            jax.ShapeDtypeStruct((8, width), F32),
        ),
        in_specs=[
            pl.BlockSpec((rows, width), lambda i: (i, 0)),
            pl.BlockSpec(gains.shape, lambda i: (0, 0)),
            pl.BlockSpec((rows, ga.shape[1]), lambda i: (i, 0)),
            pl.BlockSpec((feeds, rows, HD), lambda i: (0, i, 0)),
            pl.BlockSpec(w.shape, lambda i: (0, 0, 0)),
        ],
        out_specs=(
            pl.BlockSpec((rows, width), lambda i: (i, 0)),
            pl.BlockSpec((8, width), lambda i: (0, 0)),
        ),
        compiler_params=pltpu.CompilerParams(vmem_limit_bytes=60 << 20),
        name="close_back",
    )(x, gains, ga, pre, w)


def make_shards(dp_size, tensor_size):
    groups = dp_size // TP
    every = range(dp_size)

    def swap(value, bit):
        return lax.ppermute(value, "dp", [(i, i ^ bit) for i in every])

    def swap_tensor(value):
        return lax.ppermute(value, "tensor", [(i, i ^ 1) for i in range(tensor_size)])

    def reduce_all(value, with_tensor):
        bit = 1
        while bit < dp_size:
            value = value + swap(value, bit)
            bit *= 2
        return value + swap_tensor(value) if with_tensor else value

    def shards(
        hidden_in,
        segments,
        cotangent,
        w_query,
        w_key,
        w_value,
        w_dense,
        w_up,
        w_down,
        bias_query,
        bias_key,
        bias_value,
        bias_dense,
        bias_up,
        bias_down,
        attend_gain,
        attend_shift,
        feed_gain,
        feed_shift,
    ):
        dp = lax.axis_index("dp")
        rank = dp % TP
        width = hidden_in.shape[1]
        length = hidden_in.shape[0]
        depth = w_query.shape[0]
        heads = bias_query.shape[0]
        hidden = w_up.shape[1] // TP

        small = [
            bias_query,
            bias_key,
            bias_value,
            bias_up,
            bias_dense,
            bias_down,
            attend_gain,
            attend_shift,
            feed_gain,
            feed_shift,
            segments.astype(BF),
        ]
        packed = jnp.concatenate([a.reshape(1, -1) for a in small], axis=1)
        bit = 1
        while bit < dp_size:
            other = swap(packed, bit)
            low = (dp & bit) == 0
            packed = jnp.concatenate(
                [jnp.where(low, packed, other), jnp.where(low, other, packed)], axis=0
            )
            bit *= 2
        offset, whole = 0, []
        for a in small:
            n = a.size
            v = packed[:, offset : offset + n]
            offset += n
            if a.ndim == 1:
                whole.append(v.reshape(1, -1).astype(F32))
            else:
                v = v.reshape((dp_size,) + a.shape).transpose(1, 0, 2)
                whole.append(v.reshape(a.shape[0], -1).astype(F32))
        q_bias, k_bias, v_bias, up_bias, dense_bias, down_bias = whole[:6]
        head = lambda a: lax.dynamic_slice_in_dim(a, rank * (heads // TP), heads // TP, 0)
        up_here = lax.dynamic_slice_in_dim(up_bias.reshape(1, -1), rank * hidden, hidden, 1)
        bias = jnp.concatenate([head(a) for a in (q_bias, k_bias, v_bias)] + [up_here], axis=1)
        gain_a, shift_a, gain_f, shift_f = whole[6:10]
        norms = jnp.concatenate([gain_a, shift_a, gain_f, shift_f] * 2, axis=0)
        rows = whole[10].reshape(dp_size, length)
        seg = jnp.concatenate(
            [lax.dynamic_slice_in_dim(rows, dp ^ k, 1, 0) for k in range(TP)], axis=0
        )

        starts = jnp.zeros(seg.shape, F32)
        for value in range(1, 4):
            before = jnp.sum((seg < value).astype(F32), axis=1, keepdims=True)
            starts = jnp.where(seg == value, before, starts)
        positions = jnp.arange(length, dtype=jnp.int32).astype(F32)[None, :] - starts
        steps_in = jnp.arange(ROT // 2).astype(F32)
        inverse_freq = 10000.0 ** (-2.0 * steps_in / ROT)
        angles = positions.reshape(-1)[:, None] * inverse_freq[None, :]
        rest = jnp.zeros((angles.shape[0], LANES - ROT), F32) + starts.reshape(-1, 1)
        table = jnp.concatenate([jnp.cos(angles), jnp.sin(angles), rest], axis=1)

        weights = (w_query, w_key, w_value, w_dense.T, w_up, w_down.T)
        x_all, w_all, ga, act, pre, back, sums, _, _ = run_main(
            groups, hidden_in, cotangent, weights, norms, bias, table
        )
        x_all = x_all.reshape(TP * length, width)

        def home(partial):
            n = partial.shape[0] // TP
            mine = jnp.concatenate([partial[:n], partial[2 * n : 3 * n]], axis=0)
            theirs = jnp.concatenate([partial[n : 2 * n], partial[3 * n :]], axis=0)
            got = swap(theirs, 1)
            summed = (mine.astype(F32) + got.astype(F32)).astype(BF)
            got = swap(summed[n:], 2)
            summed = lax.optimization_barrier(
                (summed[:n].astype(F32) + got.astype(F32)).astype(BF)
            )
            return summed.astype(F32) + swap_tensor(summed).astype(F32)

        out = home(close_out(ga, act, w_all, 256))
        gains = jnp.concatenate([gain_a, gain_f], axis=0)
        h_part, norm_sums = close_back(x_all, gains, ga, pre, w_all, 256)
        h = home(h_part)
        hidden_out = (hidden_in.astype(F32) + out + (dense_bias + down_bias)).astype(BF)
        hat, inverse = normed_hat(hidden_in.astype(F32))
        grad_top = cotangent.astype(F32)
        grad_input = grad_top + inverse * (
            h
            - jnp.mean(h, axis=-1, keepdims=True)
            - hat * jnp.mean(h * hat, axis=-1, keepdims=True)
        )

        bias_grad = jnp.sum(grad_top, axis=0, keepdims=True)
        common = jnp.concatenate([norm_sums[:4].reshape(1, -1), bias_grad * 0.5], axis=1)
        local = sums[:1]
        slots = jnp.where(
            (lax.broadcasted_iota(jnp.int32, (TP, 1), 0) == rank), local, 0.0
        )
        common = reduce_all(common, True)
        slots = reduce_all(slots, False)

        def mine(vector):
            return lax.dynamic_slice_in_dim(vector, dp * depth, depth, 1).reshape(-1)

        vec = [mine(common[:, i * width : (i + 1) * width]) for i in range(5)]
        cols = bias_query.shape[1]
        my_cols = lambda a: lax.dynamic_slice_in_dim(a, dp * cols, cols, 1)
        out_bias_query = my_cols(slots[:, :HD])
        out_bias_key = slots[:, HD : HD + ROT]
        out_bias_value = my_cols(slots[:, 2 * HD : 3 * HD])
        out_bias_up = my_cols(slots[:, 3 * HD :].reshape(-1, HD))

        if back.shape[-1] != depth:
            back = lax.dynamic_slice_in_dim(back, rank * depth, depth, 3)
        back = jnp.concatenate(
            [lax.dynamic_slice_in_dim(back, rank ^ k, 1, 0) for k in range(TP)], axis=0
        )
        order = [0, 1] + list(range(4, back.shape[1]))
        units = lambda v: v.astype(F32).reshape(-1, depth)
        out_query = units(back[:, 2, :HD]).T
        out_key = units(back[:, 2, HD:]).T
        out_value = units(back[:, 3, :HD]).T
        out_dense = units(back[:, 3, HD:])
        feeds = jnp.concatenate([back[:, b : b + 1] for b in order], axis=1)
        out_up = units(feeds[:, :, :HD]).T
        out_down = units(feeds[:, :, HD:])

        return (
            hidden_out,
            grad_input,
            out_query,
            out_key,
            out_value,
            out_dense,
            out_up,
            out_down,
            out_bias_query,
            out_bias_key,
            out_bias_value,
            vec[4],
            out_bias_up,
            vec[4],
            vec[0],
            vec[1],
            vec[2],
            vec[3],
        )

    return shards


def solution(mesh):
    shards = make_shards(mesh.shape["dp"], mesh.shape["tensor"])
    in_specs = (
        P("dp", None),
        P("dp", None),
        P("dp", None),
        P("dp", "tensor"),
        P("dp", "tensor"),
        P("dp", "tensor"),
        P("tensor", "dp"),
        P("dp", "tensor"),
        P("tensor", "dp"),
        P("tensor", "dp"),
        P("tensor", "dp"),
        P("tensor", "dp"),
        P("dp"),
        P("tensor", "dp"),
        P("dp"),
        P("dp"),
        P("dp"),
        P("dp"),
        P("dp"),
    )
    out_specs = (
        P("dp", None),
        P("dp", None),
        P("dp", "tensor"),
        P("dp", "tensor"),
        P("dp", "tensor"),
        P("tensor", "dp"),
        P("dp", "tensor"),
        P("tensor", "dp"),
        P("tensor", "dp"),
        P("tensor", None),
        P("tensor", "dp"),
        P("dp"),
        P("tensor", "dp"),
        P("dp"),
        P("dp"),
        P("dp"),
        P("dp"),
        P("dp"),
    )
    return jax.shard_map(shards, mesh=mesh, in_specs=in_specs, out_specs=out_specs, check_vma=False)
```

```python
import functools

import jax
import jax.numpy as jnp
from jax import lax
from jax.experimental import pallas as pl
from jax.experimental.pallas import tpu as pltpu
from jax.sharding import PartitionSpec as P

HD = 256
ROT = 64
TP = 4
LANES = 128
BC = 2 * HD
BF = jnp.bfloat16
F32 = jnp.float32
MESH = pl.DeviceIdType.MESH
OWN_SLOTS = 4
W_SLOTS = 3
TILE = 256


def dot_nn(a, b):
    return lax.dot_general(a, b, (((1,), (0,)), ((), ())), preferred_element_type=F32)


def dot_nt(a, b):
    return lax.dot_general(a, b, (((1,), (1,)), ((), ())), preferred_element_type=F32)


def dot_tn(a, b):
    return lax.dot_general(a, b, (((0,), (0,)), ((), ())), preferred_element_type=F32)


def normed_hat(x):
    mean = jnp.mean(x, axis=-1, keepdims=True)
    centred = x - mean
    inverse = lax.rsqrt(jnp.mean(centred * centred, axis=-1, keepdims=True) + 1e-05)
    return centred * inverse, inverse


def swap_halves(u):
    half = ROT // 2
    lane = lax.broadcasted_iota(jnp.int32, u.shape, 1)
    return jnp.where(lane < half, pltpu.roll(u, LANES - half, 1), pltpu.roll(u, half, 1))


def turn(u, cosine, sine):
    head = u[:, :LANES]
    return jnp.concatenate([head * cosine + swap_halves(head) * sine, u[:, LANES:]], axis=1)


def attend(normed, cot, w_qk, w_vd, bias, table):
    scale = HD ** (-0.5)
    tokens = normed.shape[0]
    q = dot_nn(normed, w_qk[:, :HD]) + bias[:, :HD]
    k = dot_nn(normed, w_qk[:, HD:]) + bias[:, HD : 2 * HD]
    v_low = (dot_nn(normed, w_vd[:, :HD]) + bias[:, 2 * HD :]).astype(BF)
    grad_att = dot_nn(cot, w_vd[:, HD:]).astype(BF)
    half = ROT // 2
    lane = lax.broadcasted_iota(jnp.int32, table.shape, 1)
    later, sooner = pltpu.roll(table, half, 1), pltpu.roll(table, LANES - half, 1)
    cosine = jnp.where(lane < half, table, jnp.where(lane < ROT, later, 1.0))
    sine = jnp.where(lane < half, -sooner, jnp.where(lane < ROT, table, 0.0))
    start = table[:, ROT : ROT + 1].astype(jnp.int32)
    q_rot = turn(q, cosine, sine).astype(BF)
    k_rot = turn(k, cosine, sine).astype(BF)
    size = tokens // 2
    attended, grad_q, grad_k, grad_v = [], [], None, None
    for first in range(0, tokens, size):
        end = first + size
        mine = slice(first, end)
        scores = dot_nt(q_rot[mine], k_rot[:end]) * scale
        row = lax.broadcasted_iota(jnp.int32, (size, end), 0) + first
        col = lax.broadcasted_iota(jnp.int32, (size, end), 1)
        allowed = (col <= row) & (col >= start[mine])
        scores = jnp.where(allowed, scores, -1e30)
        top = jnp.max(scores, axis=-1, keepdims=True)
        weights = jnp.exp(scores - top)
        probs = weights / jnp.sum(weights, axis=-1, keepdims=True)
        probs_low = probs.astype(BF)
        attended.append(dot_nn(probs_low, v_low[:end]).astype(BF))
        grad_probs = dot_nt(grad_att[mine], v_low[:end])
        delta = jnp.sum(probs * grad_probs, axis=-1, keepdims=True)
        grad_scores = (probs * (grad_probs - delta)).astype(BF)
        grad_q.append(dot_nn(grad_scores, k_rot[:end]))
        more_k, more_v = dot_tn(grad_scores, q_rot[mine]), dot_tn(probs_low, grad_att[mine])
        if grad_k is not None:
            more_k = jnp.concatenate([more_k[:first] + grad_k, more_k[first:]], axis=0)
            more_v = jnp.concatenate([more_v[:first] + grad_v, more_v[first:]], axis=0)
        grad_k, grad_v = more_k, more_v
    grad_q = jnp.concatenate(grad_q, axis=0)
    grad_q = turn(grad_q * scale, cosine, -sine).astype(BF)
    grad_k = turn(grad_k * scale, cosine, -sine).astype(BF)
    return grad_q, grad_k, grad_v.astype(BF), jnp.concatenate(attended, axis=0)


(
    A2A_START,
    A2A_WAIT,
    TOK_START,
    TOK_Y,
    TOK_CORE,
    TOK_WAIT,
    TAB_START,
    TAB_CORE,
    TAB_WAIT,
    PK,
    PK_NORM,
    PK_BIAS,
    NORM,
    AG,
    AG_FINISH,
    LOAD,
    LOAD_WAIT,
    FF_FWD,
    FF_BWD,
    ATTN_ROW,
    ATTN_BWD,
    BIAS_SUM,
    RS,
    RS_FINISH,
    RS_DRAIN,
    CLOSE_LOAD,
    CLOSE,
    MERGE,
    SV,
) = range(29)

PLAN = (
    (A2A_START, 1),
    (A2A_START, 2),
    (PK, 0),
    (PK, 1),
    (A2A_WAIT, 1),
    (AG, 1, 1),
    (A2A_WAIT, 2),
    (AG, 2, 1),
    (A2A_START, 3),
    (PK, 2),
    (A2A_START, 4),
    (TAB_START,),
    (A2A_START, 0),
    (TOK_START, 0),
    (AG, 2, 2),
    (A2A_WAIT, 0),
    (AG, 0, 1),
    (AG, 2, 3),
    (A2A_START, 5),
    (TOK_WAIT, 0, 1),
    (PK, 3),
    (AG, 0, 2),
    (TOK_Y, 0, 0),
    (TOK_Y, 0, 1),
    (AG_FINISH, 2),
    (TOK_START, 1),
    (AG, 0, 3),
    (AG, 1, 2),
    (PK_NORM,),
    (NORM, 1),
    (PK_BIAS,),
    (TOK_Y, 1, 0),
    (AG_FINISH, 0),
    (A2A_WAIT, 3),
    (NORM, 0),
    (TOK_CORE, 0),
    (TOK_WAIT, 0, 3),
    (AG, 1, 3),
    (AG, 3, 1),
    (NORM, 2),
    (TOK_Y, 1, 1),
    (A2A_WAIT, 4),
    (LOAD, 0),
    (LOAD_WAIT, 0),
    (AG, 3, 2),
    (A2A_WAIT, 5),
    (AG_FINISH, 1),
    (TOK_WAIT, 1, 1),
    (AG, 3, 3),
    (AG, 4, 1),
    (TOK_WAIT, 1, 0),
    (NORM, 3),
    (AG, 4, 2),
    (TOK_CORE, 1),
    (LOAD, 2),
    (TOK_WAIT, 1, 3),
    (TAB_CORE,),
    (AG, 5, 1),
    (FF_FWD, 0),
    (LOAD, 1),
    (FF_BWD, 0),
    (LOAD_WAIT, 1),
    (RS, 0, 1),
    (TAB_WAIT,),
    (RS, 0, 2),
    (LOAD_WAIT, 2),
    (BIAS_SUM,),
    (FF_FWD, 1),
    (AG_FINISH, 3),
    (FF_BWD, 1),
    (LOAD, 3),
    (RS, 1, 1),
    (RS, 1, 2),
    (AG, 5, 2),
    (LOAD_WAIT, 3),
    (AG, 4, 3),
    (ATTN_ROW, 0),
    (ATTN_ROW, 1),
    (ATTN_ROW, 2),
    (ATTN_ROW, 3),
    (ATTN_BWD, 2),
    (RS, 2, 1),
    (ATTN_BWD, 3),
    (RS, 3, 1),
    (AG, 5, 3),
    (RS, 0, 3),
    (AG_FINISH, 4),
    (LOAD, 4),
    (RS, 1, 3),
    (LOAD_WAIT, 4),
    (CLOSE_LOAD, 1),
    (FF_FWD, 4),
    (CLOSE_LOAD, 0),
    (AG_FINISH, 5),
    (LOAD, 5),
    (LOAD_WAIT, 5),
    (RS, 3, 2),
    (CLOSE_LOAD, 4),
    (CLOSE_LOAD, 5),
    (FF_FWD, 5),
    (CLOSE, 0, 3, 0),
    (RS_FINISH, 0),
    (RS, 2, 2),
    (RS_DRAIN, 0),
    (CLOSE, 0, 3, 1),
    (CLOSE, 0, 2, 0),
    (FF_BWD, 4),
    (RS_FINISH, 1),
    (RS_DRAIN, 1),
    (FF_BWD, 5),
    (CLOSE, 0, 1, 0),
    (RS, 5, 1),
    (CLOSE, 1, 1, 0),
    (CLOSE, 0, 0, 0),
    (CLOSE, 0, 1, 1),
    (MERGE, 0, 0, 0),
    (RS, 4, 1),
    (CLOSE, 0, 2, 1),
    (CLOSE, 1, 3, 0),
    (CLOSE, 0, 0, 1),
    (MERGE, 0, 0, 1),
    (RS, 3, 3),
    (CLOSE, 1, 3, 1),
    (CLOSE, 1, 2, 0),
    (RS, 5, 2),
    (MERGE, 0, 1, 0),
    (CLOSE, 1, 1, 1),
    (MERGE, 0, 1, 1),
    (RS_FINISH, 3),
    (RS, 2, 3),
    (CLOSE, 1, 2, 1),
    (RS, 4, 2),
    (CLOSE, 1, 0, 0),
    (MERGE, 1, 0, 0),
    (CLOSE, 1, 0, 1),
    (RS, 5, 3),
    (SV, 0),
    (SV, 1),
    (MERGE, 1, 0, 1),
    (MERGE, 1, 1, 0),
    (RS, 4, 3),
    (RS_FINISH, 2),
    (RS_FINISH, 5),
    (SV, 2),
    (MERGE, 1, 1, 1),
    (RS_FINISH, 4),
    (SV, 3),
    (SV, 4),
    (SV, 5),
)


def make_schedule(groups):
    last = groups - 1
    spans = {1: (1,), 2: range(2, last), 3: range(max(2, last), groups)}
    rounds = (groups * TP).bit_length() - 1
    small = {0: (0,), 1: (1,), 2: (2,), 3: range(3, rounds), 4: (rounds,), 5: (rounds + 1,)}
    plan = []
    for step in PLAN:
        if step[0] in (AG, RS):
            plan += [step[:2] + (s,) for s in spans[step[2]]]
        elif step[0] in (PK, SV):
            plan += [(step[0], n) for n in small[step[1]]]
        else:
            plan.append(step)
    return plan


def main_kernel(cfg, *refs):
    groups, part, depth, width, tokens, length, feeds, back, hidden, bias_cols = cfg
    blocks = feeds + 2
    feed_of = {b: i for i, b in enumerate([0, 1] + list(range(4, blocks)))}
    dp_size = groups * TP
    rounds = dp_size.bit_length() - 1
    (
        x_in,
        cot_in,
        w_query,
        w_key,
        w_value,
        dense_t,
        w_up,
        down_t,
        table_in,
        pack_in,
        x_all,
        w_all,
        g_query,
        g_key,
        g_value,
        g_dense,
        g_up,
        g_down,
        pack,
        mine_out,
        other_out,
        sums_out,
        from_left,
        from_right,
        core_in,
        cross_in,
        big,
        wv,
        own,
        fin,
        fin_t,
        ld,
        xs,
        act_v,
        ga_v,
        table,
        norms,
        bias,
        sv,
        sv_in,
        a2a_s,
        a2a_r,
        tok_s,
        tok_r,
        ag_s,
        ag_r,
        rs_s,
        rs_r,
        bk_s,
        bk_r,
        pk_s,
        pk_r,
        sv_s,
        sv_r,
        cl_s,
        cl_r,
        cr_s,
        cr_r,
        ty_s,
        ty_r,
        ke_s,
        loc,
        stage,
    ) = refs
    dp, ty = lax.axis_index("dp"), lax.axis_index("tensor")
    rank, z = lax.rem(dp, TP), lax.div(dp, TP)
    half_rows = length // 2
    chunk = half_rows // 2

    def remote(src, dst, ssem, rsem, target, tensor=None):
        return pltpu.make_async_remote_copy(
            src_ref=src,
            dst_ref=dst,
            send_sem=ssem,
            recv_sem=rsem,
            device_id=(target, ty if tensor is None else tensor),
            device_id_type=MESH,
        )

    peer = [dp] + [lax.bitwise_xor(dp, k) for k in range(1, TP)]
    prank = [rank] + [lax.bitwise_xor(rank, k) for k in range(1, TP)]
    step_of = (TP, -TP)

    def neighbour(way):
        return lax.rem(dp + step_of[way] + dp_size, dp_size)

    def local(src, dst, sem):
        return pltpu.make_async_copy(src, dst, sem)

    def sources(b):
        if b == 2:
            return ((w_query, HD, 0), (w_key, HD, 0))
        if b == 3:
            return ((w_value, HD, 0), (dense_t, HD, 0))
        i = feed_of[b]
        return ((w_up, hidden, i * HD), (down_t, hidden, i * HD))

    def a2a_copy(b, k, half, receiving):
        array, size, offset = sources(b)[half]
        cols = pl.ds(pl.multiple_of(prank[k] * size + offset, LANES), HD)
        owner = prank[k] if receiving else rank
        rows = pl.ds(pl.multiple_of(z * part + owner * depth, depth), depth)
        dst = w_all.at[b, rows, pl.ds(half * HD, HD)]
        if k == 0:
            return local(array.at[:, cols], dst, a2a_r.at[b, k, half])
        return remote(
            array.at[:, cols], dst, a2a_s.at[b, k, half], a2a_r.at[b, k, half], peer[k]
        )

    def a2a_start(b):
        for k in (2, 3, 1, 0):
            for half in range(2):
                a2a_copy(b, k, half, False).start()

    def a2a_wait(b):
        for k in range(TP):
            for half in range(2):
                copy = a2a_copy(b, k, half, True)
                if k == 0:
                    copy.wait()
                else:
                    copy.wait_recv()

    def tok_at(which, k):
        return x_all.at[k] if which == 0 else big.at[2, pl.ds(k * length, length), :]

    def tok_rows(ref, tensor, c):
        return ref.at[pl.ds(pl.multiple_of(tensor * half_rows + c * chunk, chunk), chunk), :]

    def tok_own(which):
        src = (x_in, cot_in)[which]
        return local(src, tok_at(which, 0), tok_r.at[which, 0])

    def tok_beside(which):
        src = (x_in, cot_in)[which]
        return remote(src, tok_at(which, 1), tok_s.at[which, 1], tok_r.at[which, 1], peer[1])

    def tok_cross(which, c):
        src = (x_in, cot_in)[which]
        return remote(
            tok_rows(src, ty, c),
            tok_rows(tok_at(which, 2), ty, c),
            tok_s.at[which, 2 + c],
            tok_r.at[which, 2 + c],
            peer[2],
        )

    def tok_tensor(which, c, receiving=False):
        rows = tok_rows(tok_at(which, 2), 1 - ty if receiving else ty, c)
        return remote(
            rows, rows, tok_s.at[which, 4 + c], tok_r.at[which, 4 + c], dp, tensor=1 - ty
        )

    def tok_last(which):
        return remote(
            tok_at(which, 2), tok_at(which, 3), tok_s.at[which, 6], tok_r.at[which, 6], peer[1]
        )

    def tok_start(which):
        for c in range(2):
            tok_cross(which, c).start()
        tok_beside(which).start()
        tok_own(which).start()

    def tok_y(which, c):
        tok_cross(which, c).wait_recv()
        tok_tensor(which, c).start()

    def tok_core(which):
        for c in range(2):
            tok_tensor(which, c, True).wait_recv()
        tok_last(which).start()

    def tok_sent(which):
        for c in range(2):
            tok_tensor(which, c).wait_send()
        tok_last(which).wait_send()

    def tok_wait(which, k):
        if k == 0:
            tok_own(which).wait()
        elif k == 1:
            tok_beside(which).wait_recv()
        else:
            tok_last(which).wait_recv()

    def tab_copy(hop):
        at = lambda k: table.at[pl.ds(k * length, length), :]
        if hop == 0:
            return local(table_in, at(0), tok_r.at[2, 0])
        if hop == 3:
            return remote(at(2), at(3), tok_s.at[2, 3], tok_r.at[2, 3], peer[1])
        return remote(table_in, at(hop), tok_s.at[2, hop], tok_r.at[2, hop], peer[hop])

    def tab_start():
        for hop in (2, 1, 0):
            tab_copy(hop).start()

    def tab_core():
        tab_copy(2).wait_recv()
        tab_copy(3).start()

    def tab_wait():
        tab_copy(0).wait()
        tab_copy(1).wait_recv()
        tab_copy(3).wait_recv()

    def pk_copy(n, receiving=False):
        count = 1 << n
        other = lax.bitwise_xor(dp, count)
        first = lax.div(other if receiving else dp, count) * count
        at = pack.at[pl.ds(first, count)]
        return remote(at, at, pk_s.at[n], pk_r.at[n], other)

    def pk(n):
        if n == 0:
            copy = local(pack_in, pack.at[dp], loc.at[0])
            copy.start()
            copy.wait()
        else:
            pk_copy(n - 1, True).wait_recv()
        pk_copy(n).start()

    def pk_norm():
        pk_copy(rounds - 1, True).wait_recv()
        for j in range(dp_size):
            norms[0:4, j * depth : (j + 1) * depth] = pack[j, 0:4, 0:depth]

    def pk_bias():
        for j in range(dp_size):
            lanes = lambda i: pl.ds(i * HD + j * bias_cols, bias_cols)
            for i in range(3):
                bias[0:1, lanes(i)] = pack[j, pl.ds(8 + 4 * i + rank, 1), 0:bias_cols]
            for i in range(feeds):
                bias[0:1, lanes(3 + i)] = pack[j, pl.ds(20 + feeds * rank + i, 1), 0:bias_cols]

    def x_load(k, h, buffer):
        src = x_in if k == 0 else x_all.at[k]
        return local(src.at[pl.ds(h * TILE, TILE), :], xs.at[buffer], loc.at[buffer])

    def norm_slot(k):
        rows = min(32, TILE)
        x_load(k, 0, 0).start()
        for h in range(length // TILE):
            x_load(k, h, h % 2).wait()
            if (h + 1) * TILE < length:
                x_load(k, h + 1, (h + 1) % 2).start()

            def body(i, carry):
                at = pl.ds(pl.multiple_of(i * rows, rows), rows)
                hat, _ = normed_hat(xs[h % 2, at, :].astype(F32))
                to = pl.ds(pl.multiple_of(k * length + h * TILE + i * rows, rows), rows)
                big[0, to, :] = (hat * norms[0:1, :] + norms[1:2, :]).astype(BF)
                big[1, to, :] = (hat * norms[2:3, :] + norms[3:4, :]).astype(BF)
                return carry

            lax.fori_loop(0, TILE // rows, body, 0)

    def ag_copy(b, s, way, g):
        at = w_all.at[b, pl.ds(pl.multiple_of(g * part, part), part), :]
        return remote(at, at, ag_s.at[b, s, way], ag_r.at[b, s, way], neighbour(way))

    def ag_conditions(s):
        return ((z >= s - 1) & (z <= groups - 2), (z <= groups - s) & (z >= 1))

    def ag_step(b, s):
        go = ag_conditions(s)
        for way in range(2):
            g = (z - s + 1, z + s - 1)[way]

            @pl.when(go[way])
            def _():
                if s > 1:
                    ag_copy(b, s - 1, way, g).wait_recv()
                ag_copy(b, s, way, g).start()

    def ag_finish(b):
        @pl.when(z == groups - 1)
        def _():
            for s in range(1, groups):
                ag_copy(b, s, 0, z - s).wait_recv()

        @pl.when(z == 0)
        def _():
            for s in range(1, groups):
                ag_copy(b, s, 1, z + s).wait_recv()

    def ag_drain(b):
        for s in range(1, groups):
            go = ag_conditions(s)
            for way in range(2):
                g = (z - s + 1, z + s - 1)[way]
                pl.when(go[way])(lambda: ag_copy(b, s, way, g).wait_send())

    def rs_copy(b, t, way, d):
        land = (from_left, from_right)[way]
        return remote(
            own.at[b % OWN_SLOTS, d],
            land.at[b, t - 1],
            rs_s.at[b, t, way],
            rs_r.at[b, t, way],
            neighbour(way),
        )

    rows_add = min(32, BC)

    def rs_load(b, t, way):
        return local((from_left, from_right)[way].at[b, t - 1], ld.at[way], loc.at[4 + way])

    def add_in(b, d, way):
        slot = b % OWN_SLOTS

        def body(i, carry):
            at = pl.ds(pl.multiple_of(i * rows_add, rows_add), rows_add)
            total = own[slot, d, at, :].astype(F32) + ld[way, at, :].astype(F32)
            own[slot, d, at, :] = total.astype(BF)
            return carry

        lax.fori_loop(0, BC // rows_add, body, 0)

    def rs_conditions(t):
        return (z <= t - 1, z >= groups - t)

    def rs_step(b, t):
        go = rs_conditions(t)
        ends = (z == 0, z == groups - 1)
        dest = (z + groups - t, z - groups + t)
        for way in range(2):
            d = dest[way]
            if t > 1:

                @pl.when(go[way] & jnp.logical_not(ends[way]))
                def _():
                    rs_copy(b, t - 1, way, d).wait_recv()
                    rs_load(b, t - 1, way).start()

        for way in range(2):
            d = dest[way]
            if t > 1:

                @pl.when(go[way] & jnp.logical_not(ends[way]))
                def _():
                    rs_load(b, t - 1, way).wait()
                    add_in(b, d, way)

            @pl.when(go[way])
            def _():
                rs_copy(b, t, way, d).start()

    def rs_drain(b):
        for t in range(1, groups):
            go = rs_conditions(t)
            for way in range(2):
                d = (z + groups - t, z - groups + t)[way]
                pl.when(go[way])(lambda: rs_copy(b, t, way, d).wait_send())

    def results(b, half):
        if b == 2:
            return ((g_query, g_key)[half], HD, 0, True)
        if b == 3:
            return ((g_value, g_dense)[half], HD, 0, half == 0)
        return ((g_up, g_down)[half], hidden, feed_of[b] * HD, half == 0)

    def bk_copy(b, k, half, receiving=False):
        array, size, offset, turned = results(b, half)
        owner = prank[k] if receiving else rank
        at = pl.ds(pl.multiple_of(owner * size + offset, LANES), HD)
        if turned:
            rows = pl.ds(pl.multiple_of(prank[k] * depth, depth), depth)
            src, dst = fin_t.at[b % 2, half, rows, :], array.at[:, at]
        else:
            src, dst = fin.at[b % 2], array.at[at, :]
            if back != part:
                src = src.at[:, pl.ds(pl.multiple_of(prank[k] * depth, LANES), depth)]
        if k == 0:
            return local(src, dst, bk_r.at[b, k, half])
        return remote(src, dst, bk_s.at[b, k, half], bk_r.at[b, k, half], peer[k])

    def bk_drain(b):
        for half in range(2):
            bk_copy(b, 0, half).wait()
            for k in range(1, TP):
                bk_copy(b, k, half).wait_send()

    def rs_finish(b):
        last = groups - 1
        inner = (z > 0, z < groups - 1)
        for way in range(2):

            @pl.when(inner[way])
            def _():
                rs_copy(b, last, way, z).wait_recv()
                rs_load(b, last, way).start()

        if b >= 2:
            bk_drain(b - 2)
        for way in range(2):
            pl.when(inner[way])(lambda: rs_load(b, last, way).wait())

        slot = b % OWN_SLOTS
        for half in range(2):
            turned = results(b, half)[3]

            def body(i, carry):
                unit = pl.multiple_of(i * LANES, LANES)
                at = pl.ds(half * HD + unit, LANES)
                total = own[slot, z, at, :].astype(F32)
                for way in range(2):
                    total += jnp.where(inner[way], ld[way, at, :].astype(F32), 0.0)
                if turned:
                    fin_t[b % 2, half, :, pl.ds(unit, LANES)] = total.T.astype(BF)
                else:
                    fin[b % 2, pl.ds(unit, LANES), :] = total.astype(BF)
                return carry

            lax.fori_loop(0, HD // LANES, body, 0)
        for k in (2, 3, 1, 0):
            for half in range(2):
                bk_copy(b, k, half).start()

    slot_qk, slot_vd = 2, 0
    slot_of = {0: 0, 1: 1, 2: slot_qk, 3: slot_vd, 4: 1, 5: 1}

    def w_load(b):
        return local(w_all.at[b], wv.at[slot_of[b]], loc.at[6 + slot_of[b]])

    def feed_forward(b):
        i = feed_of[b]
        slot = slot_of[b]
        lanes = slice(i * HD, (i + 1) * HD)

        def body(n, carry):
            at = pl.ds(pl.multiple_of(n * TILE, TILE), TILE)
            pre = dot_nn(big[1, at, :], wv[slot, :, :HD]) + bias[0:1, (3 + i) * HD : (4 + i) * HD]
            grad_act = dot_nn(big[2, at, :], wv[slot, :, HD:])
            cdf = 0.5 * (1.0 + lax.erf(pre * 0.7071067811865476))
            pdf = jnp.exp(-0.5 * pre * pre) * 0.3989422804014327
            act_v[0, at, lanes] = (pre * cdf).astype(BF)
            grad_pre = (grad_act * (cdf + pre * pdf)).astype(BF)
            act_v[1, at, lanes] = grad_pre
            return carry + jnp.sum(grad_pre.astype(F32), axis=0, keepdims=True)

        total = lax.fori_loop(0, tokens // TILE, body, jnp.zeros((1, HD), F32))
        sv[0, pl.ds(8 + rank, 1), (3 + i) * HD : (4 + i) * HD] = total

    def feed_backward(b):
        slot = b % OWN_SLOTS
        i = feed_of[b]
        lanes = slice(i * HD, (i + 1) * HD)

        def body(d, carry):
            cols = pl.ds(pl.multiple_of(d * part, part), part)
            own[slot, d, :HD, :] = dot_tn(act_v[1, :, lanes], big[1, :, cols]).astype(BF)
            own[slot, d, HD:, :] = dot_tn(act_v[0, :, lanes], big[2, :, cols]).astype(BF)
            return carry

        lax.fori_loop(0, groups, body, 0)

    def attention(between):
        def body(n, carry):
            at = pl.ds(pl.multiple_of(n * length, length), length)
            grads = attend(
                big[0, at, :],
                big[2, at, :],
                wv.at[slot_qk],
                wv.at[slot_vd],
                bias[0:1, : 3 * HD],
                table[at, :],
            )
            for j, g in enumerate(grads):
                ga_v[at, j * HD : (j + 1) * HD] = g
            sums = [jnp.sum(g.astype(F32), axis=0, keepdims=True) for g in grads[:3]]
            carry = carry + jnp.concatenate(sums, axis=1)
            for j, some in enumerate(between):
                if some:

                    @pl.when(n == j)
                    def _():
                        for step in some:
                            run(step)

            return carry

        total = lax.fori_loop(0, TP, body, jnp.zeros((1, 3 * HD), F32))
        sv[0, pl.ds(8 + rank, 1), : 3 * HD] = total

    def attention_back(b):
        slot = b % OWN_SLOTS

        def body(d, carry):
            cols = pl.ds(pl.multiple_of(d * part, part), part)
            if b == 2:
                own[slot, d, :HD, :] = dot_tn(ga_v[:, :HD], big[0, :, cols]).astype(BF)
                own[slot, d, HD:, :] = dot_tn(ga_v[:, HD:BC], big[0, :, cols]).astype(BF)
            else:
                own[slot, d, :HD, :] = dot_tn(ga_v[:, BC : 3 * HD], big[0, :, cols]).astype(BF)
                own[slot, d, HD:, :] = dot_tn(ga_v[:, 3 * HD :], big[2, :, cols]).astype(BF)
            return carry

        lax.fori_loop(0, groups, body, 0)

    def bias_sum():
        rows = min(64, length)

        def body(i, carry):
            at = pl.ds(pl.multiple_of(i * rows, rows), rows)
            return carry + jnp.sum(big[2, at, :].astype(F32), axis=0, keepdims=True)

        total = lax.fori_loop(0, length // rows, body, jnp.zeros((1, width), F32))
        sv[0, 4:5, :] = total * 0.5

    def close_weights(b, half):
        i = feed_of[b]
        lanes = pl.ds((feeds if half == 0 else 0) * HD + i * HD, HD)
        return local(
            w_all.at[b, :, pl.ds(half * HD, HD)], big.at[0, :, lanes], loc.at[9 + 2 * i + half]
        )

    def close_load(b):
        for half in range(2):
            close_weights(b, half).start()

    def close_ready(half):
        for b in feed_of:
            close_weights(b, half).wait()

    sub = TILE // 2

    def staged(q, k, row, count):
        if q == 0 and k == 2:
            return stage.at[pl.ds(row, count), :]
        return big.at[1 + q, pl.ds(k * length + row, count), :]

    span = min(BC, width)

    def staged_part(q, k, h, i):
        if q == 0 and k == 3:
            rows = pl.ds(pl.multiple_of(i * length + h * TILE, TILE), TILE)
            return wv.at[slot_of[blocks - 1], rows, pl.ds(0, span)]
        cols = pl.ds(pl.multiple_of(i * span, span), span)
        return staged(q, k, h * TILE, TILE).at[:, cols]

    def close_copy(q, k, h, i):
        rows = pl.ds(h * TILE, TILE)
        return remote(
            staged_part(q, k, h, i),
            core_in.at[q, k // 2, rows, pl.ds(i * span, span)],
            cl_s.at[q, k, h, i],
            cl_r.at[q, k, h, i],
            peer[1],
        )

    spans = range(width // span)

    def cross_copy(q, h, c):
        rows = pl.ds(h * TILE + c * sub, sub)
        return remote(
            staged(q, 2, h * TILE + c * sub, sub),
            cross_in.at[q, rows, :],
            cr_s.at[q, h, c],
            cr_r.at[q, h, c],
            peer[2],
        )

    def tensor_copy(q, h, c):
        rows = pl.ds(h * TILE + c * sub, sub)
        return remote(
            staged(q, 0, h * TILE + c * sub, sub),
            other_out.at[q, rows, :],
            ty_s.at[q, h, c],
            ty_r.at[q, h, c],
            dp,
            tensor=1 - ty,
        )

    def keep_copy(q, h, c):
        rows = pl.ds(h * TILE + c * sub, sub)
        return local(staged(q, 0, h * TILE + c * sub, sub), mine_out.at[q, rows, :], ke_s.at[q, h, c])

    def merge(q, h, c):
        cross_copy(q, h, c).wait_recv()
        rows = pl.ds(h * TILE + c * sub, sub)
        copy = local(cross_in.at[q, rows, :], xs.at[1, pl.ds(0, sub), :], loc.at[1])
        copy.start()
        copy.wait()
        rows_here = min(32, sub)
        mine = staged(q, 0, h * TILE + c * sub, sub)

        def body(i, carry):
            at = pl.ds(pl.multiple_of(i * rows_here, rows_here), rows_here)
            mine[at, :] = (mine[at, :].astype(F32) + xs[1, at, :].astype(F32)).astype(BF)
            return carry

        lax.fori_loop(0, sub // rows_here, body, 0)
        tensor_copy(q, h, c).start()
        keep_copy(q, h, c).start()

    ready = []

    def close(q, k, h):
        rows = pl.ds(h * TILE, TILE)
        at = slice(k * length + h * TILE, k * length + (h + 1) * TILE)
        arrived = []
        if q not in ready:
            ready.append(q)
            close_ready(1 - q)
            if q == 1:
                tok_sent(1)
        if q == 1:
            x_load(k, h, 0).start()
        if k in (0, 2):
            for i in spans:
                close_copy(q, k + 1, h, i).wait_recv()
            copy = local(core_in.at[q, k // 2, rows, :], xs.at[1], loc.at[1])
            copy.start()
            arrived.append((copy, 1))
        if q == 1:
            x_load(k, h, 0).wait()
            x = xs[0].astype(F32)
            mean = jnp.mean(x, axis=-1, keepdims=True)
            inverse = lax.rsqrt(jnp.mean(jnp.square(x - mean), axis=-1, keepdims=True) + 1e-05)
        for copy, _ in arrived:
            copy.wait()
        col = lambda v: jnp.sum(v, axis=0, keepdims=True)
        step = min(HD, span)
        per = span // step

        def body(i, carry):
            cols = pl.ds(pl.multiple_of(i * step, step), step)
            if q == 0:
                total = dot_nt(act_v[0, at, :], big[0, cols, : feeds * HD])
                total += dot_nt(ga_v[at, 3 * HD :], wv[slot_vd, cols, HD:])
            else:
                hat = (xs[0, :, cols].astype(F32) - mean) * inverse
                grad_f = dot_nt(act_v[1, at, :], big[0, cols, feeds * HD :])
                sv[0, 2:3, cols] += col(grad_f * hat)
                sv[0, 3:4, cols] += col(grad_f)
                grad_a = dot_nt(ga_v[at, :BC], wv[slot_qk, cols, :])
                grad_a += dot_nt(ga_v[at, BC : 3 * HD], wv[slot_vd, cols, :HD])
                sv[0, 0:1, cols] += col(grad_a * hat)
                sv[0, 1:2, cols] += col(grad_a)
                total = grad_f * norms[2:3, cols] + grad_a * norms[0:1, cols]
            for _, buffer in arrived:
                total += xs[buffer, :, cols].astype(F32)
            lanes = pl.ds(pl.multiple_of(lax.rem(i, per) * step, step), step)
            staged_part(q, k, h, lax.div(i, per))[:, lanes] = total.astype(BF)
            return carry

        lax.fori_loop(0, width // step, body, 0)
        if k in (1, 3):
            for i in spans:
                close_copy(q, k, h, i).start()
        if k == 2:
            for c in range(2):
                cross_copy(q, h, c).start()

    def sv_copy(n):
        if n < rounds:
            return remote(
                sv.at[n], sv_in.at[n], sv_s.at[n], sv_r.at[n], lax.bitwise_xor(dp, 1 << n)
            )
        rows = pl.ds(0, 8)
        return remote(
            sv.at[n, rows], sv_in.at[n, rows], sv_s.at[n], sv_r.at[n], dp, tensor=1 - ty
        )

    def sv_step(n):
        if n > 0:
            sv_copy(n - 1).wait_recv()
        if n <= rounds:
            if n > 0:
                sv[n] = sv[n - 1] + sv_in[n - 1]
            sv_copy(n).start()
        else:
            sums_out[0:8] = sv[rounds, 0:8] + sv_in[rounds, 0:8]
            sums_out[8:16] = sv[rounds, 8:16]

    barrier = pltpu.get_barrier_semaphore()

    def greet(target, tensor):
        pl.semaphore_signal(barrier, inc=1, device_id=(target, tensor), device_id_type=MESH)

    greet(dp, 1 - ty)
    for k in range(1, TP):
        greet(peer[k], ty)
    bit = TP
    while bit < dp_size:
        greet(lax.bitwise_xor(dp, bit), ty)
        bit *= 2
    odd = lax.rem(z, 2) == 1
    up_more, down_more = odd & (z < groups - 1), jnp.logical_not(odd) & (z > 0)
    pl.when(up_more)(lambda: greet(neighbour(0), ty))
    pl.when(down_more)(lambda: greet(neighbour(1), ty))
    count = rounds + 2
    more = up_more | down_more
    pl.when(more)(lambda: pl.semaphore_wait(barrier, count + 1))
    pl.when(jnp.logical_not(more))(lambda: pl.semaphore_wait(barrier, count))

    steps = {
        A2A_START: a2a_start,
        A2A_WAIT: a2a_wait,
        TOK_START: tok_start,
        TOK_Y: tok_y,
        TOK_CORE: tok_core,
        TOK_WAIT: tok_wait,
        TAB_START: tab_start,
        TAB_CORE: tab_core,
        TAB_WAIT: tab_wait,
        PK: pk,
        PK_NORM: pk_norm,
        PK_BIAS: pk_bias,
        NORM: norm_slot,
        AG: ag_step,
        AG_FINISH: ag_finish,
        LOAD: lambda b: w_load(b).start(),
        LOAD_WAIT: lambda b: w_load(b).wait(),
        FF_FWD: feed_forward,
        FF_BWD: feed_backward,
        ATTN_BWD: attention_back,
        BIAS_SUM: bias_sum,
        RS: rs_step,
        RS_FINISH: rs_finish,
        RS_DRAIN: rs_drain,
        CLOSE_LOAD: close_load,
        CLOSE: close,
        MERGE: merge,
        SV: sv_step,
    }

    def run(step):
        steps[step[0]](*step[1:])

    sv[0] = jnp.zeros(sv.shape[1:], F32)
    ld[...] = jnp.zeros(ld.shape, BF)
    plan = make_schedule(groups)
    rows_at = [plan.index((ATTN_ROW, n)) for n in range(TP)]
    for step in plan[: rows_at[0]]:
        run(step)
    attention([plan[i + 1 : j] for i, j in zip(rows_at, rows_at[1:])] + [[]])
    for step in plan[rows_at[-1] + 1 :]:
        run(step)

    drained = [step[1] for step in plan if step[0] == RS_DRAIN]
    for b in range(blocks):
        for k in range(1, TP):
            for half in range(2):
                a2a_copy(b, k, half, False).wait_send()
        ag_drain(b)
        if b not in drained:
            rs_drain(b)
    tok_own(0).wait()
    for which in range(2):
        tok_beside(which).wait_send()
        for c in range(2):
            tok_cross(which, c).wait_send()
    tok_sent(0)
    for hop in (1, 2, 3):
        tab_copy(hop).wait_send()
    for n in range(rounds):
        pk_copy(n).wait_send()
    for n in range(rounds + 1):
        sv_copy(n).wait_send()
    for q in range(2):
        for h in range(length // TILE):
            for k in (1, 3):
                for i in spans:
                    close_copy(q, k, h, i).wait_send()
            for c in range(2):
                cross_copy(q, h, c).wait_send()
                tensor_copy(q, h, c).wait_send()
                tensor_copy(q, h, c).wait_recv()
                keep_copy(q, h, c).wait()
    bk_drain(blocks - 2)
    bk_drain(blocks - 1)
    for b in range(blocks):
        for k in range(1, TP):
            for half in range(2):
                bk_copy(b, k, half, True).wait_recv()


def run_main(groups, x, cot, weights, table, pack, bias_cols):
    length, width = x.shape
    depth = weights[0].shape[0]
    part = width // groups
    tokens = TP * length
    hidden = weights[4].shape[1] // TP
    feeds = hidden // HD
    blocks = feeds + 2
    dp_size = groups * TP
    rounds = dp_size.bit_length() - 1
    back = depth if depth % LANES == 0 else part
    cfg = (groups, part, depth, width, tokens, length, feeds, back, hidden, bias_cols)
    hbm = pl.BlockSpec(memory_space=pltpu.HBM)
    vmem = pl.BlockSpec(memory_space=pltpu.VMEM)
    sem = pltpu.SemaphoreType.DMA
    shape = jax.ShapeDtypeStruct
    tiles = length // TILE
    return pl.pallas_call(
        functools.partial(main_kernel, cfg),
        out_shape=(
            shape((TP, length, width), BF),
            shape((blocks, width, BC), BF),
            shape((depth, TP * HD), BF),
            shape((depth, TP * HD), BF),
            shape((depth, TP * HD), BF),
            shape((TP * HD, back), BF),
            shape((depth, TP * hidden), BF),
            shape((TP * hidden, back), BF),
            shape((dp_size,) + pack.shape, F32),
            shape((2, length, width), BF),
            shape((2, length, width), BF),
            shape((16, width), F32),
            shape((blocks, groups, BC, part), BF),
            shape((blocks, groups, BC, part), BF),
            shape((2, 2, length, width), BF),
            shape((2, length, width), BF),
        ),
        in_specs=[hbm] * 10,
        out_specs=(hbm,) * 8 + (vmem,) + (hbm,) * 2 + (vmem,) + (hbm,) * 4,
        scratch_shapes=[
            pltpu.VMEM((3, tokens, width), BF),
            pltpu.VMEM((W_SLOTS, width, BC), BF),
            pltpu.VMEM((OWN_SLOTS, groups, BC, part), BF),
            pltpu.VMEM((2, HD, part), BF),
            pltpu.VMEM((2, 2, part, HD), BF),
            pltpu.VMEM((2, BC, part), BF),
            pltpu.VMEM((2, TILE, width), BF),
            pltpu.VMEM((2, tokens, feeds * HD), BF),
            pltpu.VMEM((tokens, 4 * HD), BF),
            pltpu.VMEM((tokens, LANES), F32),
            pltpu.VMEM((8, width), F32),
            pltpu.VMEM((8, (3 + feeds) * HD), F32),
            pltpu.VMEM((rounds + 1, 16, width), F32),
            pltpu.VMEM((rounds + 1, 16, width), F32),
            sem((blocks, TP, 2)),
            sem((blocks, TP, 2)),
            sem((3, 7)),
            sem((3, 7)),
            sem((blocks, groups, 2)),
            sem((blocks, groups, 2)),
            sem((blocks, groups, 2)),
            sem((blocks, groups, 2)),
            sem((blocks, TP, 2)),
            sem((blocks, TP, 2)),
            sem((rounds,)),
            sem((rounds,)),
            sem((rounds + 1,)),
            sem((rounds + 1,)),
            sem((2, TP, tiles, width // min(BC, width))),
            sem((2, TP, tiles, width // min(BC, width))),
            sem((2, tiles, 2)),
            sem((2, tiles, 2)),
            sem((2, tiles, 2)),
            sem((2, tiles, 2)),
            sem((2, tiles, 2)),
            sem((9 + 2 * feeds,)),
            pltpu.VMEM((length, width), BF),
        ],
        compiler_params=pltpu.CompilerParams(
            collective_id=0, has_side_effects=True, vmem_limit_bytes=67043328
        ),
        name="main",
    )(x, cot, *weights, table, pack)


def make_shards(dp_size):
    groups = dp_size // TP

    def shards(
        hidden_in,
        segments,
        cotangent,
        w_query,
        w_key,
        w_value,
        w_dense,
        w_up,
        w_down,
        bias_query,
        bias_key,
        bias_value,
        bias_dense,
        bias_up,
        bias_down,
        attend_gain,
        attend_shift,
        feed_gain,
        feed_shift,
    ):
        dp = lax.axis_index("dp")
        rank = dp % TP
        length, width = hidden_in.shape
        depth = w_query.shape[0]
        cols = bias_query.shape[1]

        vectors = (attend_gain, attend_shift, feed_gain, feed_shift, bias_dense, bias_down)
        wide = lambda a: jnp.pad(a.astype(F32), ((0, 0), (0, LANES - a.shape[1])))
        pack = jnp.concatenate(
            [wide(jnp.stack(vectors + (vectors[0],) * 2))]
            + [wide(a) for a in (bias_query, bias_key, bias_value, bias_up)],
            axis=0,
        )
        pack = jnp.pad(pack, ((0, -pack.shape[0] % 8), (0, 0)))

        starts = jnp.zeros(segments.shape, jnp.int32)
        for value in range(1, 4):
            before = jnp.sum((segments < value).astype(jnp.int32), axis=1, keepdims=True)
            starts = jnp.where(segments == value, before, starts)
        positions = (jnp.arange(length, dtype=jnp.int32)[None, :] - starts).astype(F32)
        steps_in = jnp.arange(ROT // 2).astype(F32)
        inverse_freq = 10000.0 ** (-2.0 * steps_in / ROT)
        angles = positions.reshape(-1, 1) * inverse_freq[None, :]
        rest = jnp.broadcast_to(starts.reshape(-1, 1).astype(F32), (length, LANES - ROT))
        table = jnp.concatenate([jnp.cos(angles), jnp.sin(angles), rest], axis=1)

        weights = (w_query, w_key, w_value, w_dense.T, w_up, w_down.T)
        made = run_main(groups, hidden_in, cotangent, weights, table, pack, cols)
        grads, (packs, mine, other, sums) = made[2:8], made[8:12]

        biases = (packs[:, 4, :depth] + packs[:, 5, :depth]).reshape(1, -1)
        x = hidden_in.astype(F32)
        total = mine.astype(F32) + other.astype(F32)
        hidden_out = (x + total[0] + biases).astype(BF)
        hat, inverse = normed_hat(x)
        h = total[1]
        grad_input = cotangent.astype(F32) + inverse * (
            h
            - jnp.mean(h, axis=-1, keepdims=True)
            - hat * jnp.mean(h * hat, axis=-1, keepdims=True)
        )

        vec = lax.dynamic_slice_in_dim(sums[:8], dp * depth, depth, 1)
        slots = sums[8 : 8 + TP]
        my_cols = lambda a: lax.dynamic_slice_in_dim(a, dp * cols, cols, 1)
        out_bias_query = my_cols(slots[:, :HD])
        out_bias_key = slots[:, HD : HD + ROT]
        out_bias_value = my_cols(slots[:, 2 * HD : 3 * HD])
        ups = slots[:, 3 * HD : 3 * HD + w_up.shape[1] // TP]
        out_bias_up = my_cols(ups.reshape(-1, HD))

        g_query, g_key, g_value, g_dense, g_up, g_down = grads
        if g_dense.shape[1] != depth:
            g_dense, g_down = (
                lax.dynamic_slice_in_dim(g, rank * depth, depth, 1) for g in (g_dense, g_down)
            )

        return (
            hidden_out,
            grad_input,
            g_query.astype(F32),
            g_key.astype(F32),
            g_value.astype(F32),
            g_dense.astype(F32),
            g_up.astype(F32),
            g_down.astype(F32),
            out_bias_query,
            out_bias_key,
            out_bias_value,
            vec[4],
            out_bias_up,
            vec[4],
            vec[0],
            vec[1],
            vec[2],
            vec[3],
        )

    return shards


def solution(mesh):
    shards = make_shards(mesh.shape["dp"])
    in_specs = (
        P("dp", None),
        P("dp", None),
        P("dp", None),
        P("dp", "tensor"),
        P("dp", "tensor"),
        P("dp", "tensor"),
        P("tensor", "dp"),
        P("dp", "tensor"),
        P("tensor", "dp"),
        P("tensor", "dp"),
        P("tensor", "dp"),
        P("tensor", "dp"),
        P("dp"),
        P("tensor", "dp"),
        P("dp"),
        P("dp"),
        P("dp"),
        P("dp"),
        P("dp"),
    )
    out_specs = (
        P("dp", None),
        P("dp", None),
        P("dp", "tensor"),
        P("dp", "tensor"),
        P("dp", "tensor"),
        P("tensor", "dp"),
        P("dp", "tensor"),
        P("tensor", "dp"),
        P("tensor", "dp"),
        P("tensor", None),
        P("tensor", "dp"),
        P("dp"),
        P("tensor", "dp"),
        P("dp"),
        P("dp"),
        P("dp"),
        P("dp"),
        P("dp"),
    )
    return jax.shard_map(shards, mesh=mesh, in_specs=in_specs, out_specs=out_specs, check_vma=False)
```

```python
import functools

import jax
import jax.numpy as jnp
from jax import lax
from jax.experimental import pallas as pl
from jax.experimental.pallas import tpu as pltpu
from jax.sharding import PartitionSpec as P

HD = 256
ROT = 64
TP = 4
LANES = 128
BC = 2 * HD
BF = jnp.bfloat16
F32 = jnp.float32
MESH = pl.DeviceIdType.MESH
OWN_SLOTS = 4
W_SLOTS = 3
TILE = 256


def dot_nn(a, b):
    return lax.dot_general(a, b, (((1,), (0,)), ((), ())), preferred_element_type=F32)


def dot_nt(a, b):
    return lax.dot_general(a, b, (((1,), (1,)), ((), ())), preferred_element_type=F32)


def dot_tn(a, b):
    return lax.dot_general(a, b, (((0,), (0,)), ((), ())), preferred_element_type=F32)


def normed_hat(x):
    mean = jnp.mean(x, axis=-1, keepdims=True)
    centred = x - mean
    inverse = lax.rsqrt(jnp.mean(centred * centred, axis=-1, keepdims=True) + 1e-05)
    return centred * inverse, inverse


def swap_halves(u):
    half = ROT // 2
    lane = lax.broadcasted_iota(jnp.int32, u.shape, 1)
    return jnp.where(lane < half, pltpu.roll(u, LANES - half, 1), pltpu.roll(u, half, 1))


def turn(u, cosine, sine):
    head = u[:, :LANES]
    return jnp.concatenate([head * cosine + swap_halves(head) * sine, u[:, LANES:]], axis=1)


def attend(normed, cot, w_qk, w_vd, bias, table):
    scale = HD ** (-0.5)
    tokens = normed.shape[0]
    q = dot_nn(normed, w_qk[:, :HD]) + bias[:, :HD]
    k = dot_nn(normed, w_qk[:, HD:]) + bias[:, HD : 2 * HD]
    v_low = (dot_nn(normed, w_vd[:, :HD]) + bias[:, 2 * HD :]).astype(BF)
    grad_att = dot_nn(cot, w_vd[:, HD:]).astype(BF)
    half = ROT // 2
    lane = lax.broadcasted_iota(jnp.int32, table.shape, 1)
    later, sooner = pltpu.roll(table, half, 1), pltpu.roll(table, LANES - half, 1)
    cosine = jnp.where(lane < half, table, jnp.where(lane < ROT, later, 1.0))
    sine = jnp.where(lane < half, -sooner, jnp.where(lane < ROT, table, 0.0))
    start = table[:, ROT : ROT + 1].astype(jnp.int32)
    q_rot = turn(q, cosine, sine).astype(BF)
    k_rot = turn(k, cosine, sine).astype(BF)
    size = tokens // 2
    attended, grad_q, grad_k, grad_v = [], [], None, None
    for first in range(0, tokens, size):
        end = first + size
        mine = slice(first, end)
        scores = dot_nt(q_rot[mine], k_rot[:end]) * scale
        row = lax.broadcasted_iota(jnp.int32, (size, end), 0) + first
        col = lax.broadcasted_iota(jnp.int32, (size, end), 1)
        allowed = (col <= row) & (col >= start[mine])
        scores = jnp.where(allowed, scores, -1e30)
        top = jnp.max(scores, axis=-1, keepdims=True)
        weights = jnp.exp(scores - top)
        probs = weights / jnp.sum(weights, axis=-1, keepdims=True)
        probs_low = probs.astype(BF)
        attended.append(dot_nn(probs_low, v_low[:end]).astype(BF))
        grad_probs = dot_nt(grad_att[mine], v_low[:end])
        delta = jnp.sum(probs * grad_probs, axis=-1, keepdims=True)
        grad_scores = (probs * (grad_probs - delta)).astype(BF)
        grad_q.append(dot_nn(grad_scores, k_rot[:end]))
        more_k, more_v = dot_tn(grad_scores, q_rot[mine]), dot_tn(probs_low, grad_att[mine])
        if grad_k is not None:
            more_k = jnp.concatenate([more_k[:first] + grad_k, more_k[first:]], axis=0)
            more_v = jnp.concatenate([more_v[:first] + grad_v, more_v[first:]], axis=0)
        grad_k, grad_v = more_k, more_v
    grad_q = jnp.concatenate(grad_q, axis=0)
    grad_q = turn(grad_q * scale, cosine, -sine).astype(BF)
    grad_k = turn(grad_k * scale, cosine, -sine).astype(BF)
    return grad_q, grad_k, grad_v.astype(BF), jnp.concatenate(attended, axis=0)


(
    A2A_START,
    A2A_WAIT,
    TOK_START,
    TOK_Y,
    TOK_CORE,
    TOK_WAIT,
    TAB_MAKE,
    TAB_START,
    TAB_CORE,
    TAB_WAIT,
    PK,
    PK_NORM,
    PK_BIAS,
    NORM,
    AG,
    AG_FINISH,
    LOAD,
    LOAD_WAIT,
    FF_FWD,
    FF_BWD,
    ATTN_ROW,
    ATTN_BWD,
    BIAS_SUM,
    RS,
    RS_FINISH,
    RS_DRAIN,
    CLOSE_LOAD,
    CLOSE,
    MERGE,
    SV,
) = range(30)

PLAN = (
    (A2A_START, 1),
    (A2A_START, 0),
    (A2A_START, 3),
    (A2A_WAIT, 1),
    (AG, 1, 1),
    (PK, 0),
    (A2A_WAIT, 3),
    (A2A_WAIT, 0),
    (AG, 0, 1),
    (PK, 1),
    (A2A_START, 4),
    (PK, 2),
    (TOK_START, 0),
    (AG, 1, 2),
    (PK, 3),
    (TOK_START, 1),
    (AG, 1, 3),
    (A2A_START, 2),
    (AG, 3, 1),
    (TOK_Y, 0, 0),
    (TOK_WAIT, 0, 1),
    (AG_FINISH, 1),
    (TOK_WAIT, 1, 1),
    (TOK_Y, 0, 1),
    (PK_NORM,),
    (PK_BIAS,),
    (TOK_WAIT, 1, 0),
    (AG, 3, 2),
    (TOK_CORE, 0),
    (AG, 0, 2),
    (TAB_START,),
    (LOAD, 1),
    (AG, 0, 3),
    (A2A_START, 5),
    (TOK_Y, 1, 0),
    (A2A_WAIT, 2),
    (AG, 2, 1),
    (TOK_WAIT, 0, 3),
    (A2A_WAIT, 4),
    (A2A_WAIT, 5),
    (LOAD_WAIT, 1),
    (TOK_Y, 1, 1),
    (AG, 3, 3),
    (AG, 5, 1),
    (AG, 2, 2),
    (TOK_CORE, 1),
    (AG, 2, 3),
    (AG, 5, 2),
    (AG_FINISH, 0),
    (TAB_CORE,),
    (NORM, 1),
    (NORM, 0),
    (AG, 4, 1),
    (TOK_WAIT, 1, 3),
    (TAB_WAIT,),
    (LOAD, 0),
    (NORM, 2),
    (NORM, 3),
    (FF_FWD, 1),
    (LOAD_WAIT, 0),
    (AG_FINISH, 3),
    (FF_FWD, 0),
    (FF_BWD, 1),
    (RS, 1, 1),
    (AG, 4, 2),
    (FF_BWD, 0),
    (RS, 0, 1),
    (AG_FINISH, 2),
    (RS, 0, 2),
    (LOAD, 3),
    (AG, 4, 3),
    (LOAD, 2),
    (AG, 5, 3),
    (LOAD_WAIT, 2),
    (LOAD_WAIT, 3),
    (RS, 1, 2),
    (ATTN_ROW, 0),
    (ATTN_ROW, 1),
    (ATTN_ROW, 2),
    (ATTN_ROW, 3),
    (ATTN_BWD, 2),
    (RS, 1, 3),
    (RS, 2, 1),
    (ATTN_BWD, 3),
    (AG_FINISH, 4),
    (LOAD, 4),
    (BIAS_SUM,),
    (RS, 3, 1),
    (CLOSE_LOAD, 0),
    (LOAD_WAIT, 4),
    (CLOSE_LOAD, 4),
    (FF_FWD, 4),
    (AG_FINISH, 5),
    (CLOSE_LOAD, 5),
    (CLOSE_LOAD, 1),
    (RS, 0, 3),
    (LOAD, 5),
    (RS, 2, 2),
    (LOAD_WAIT, 5),
    (FF_FWD, 5),
    (RS, 3, 2),
    (CLOSE, 0, 3),
    (RS_FINISH, 1),
    (RS_DRAIN, 1),
    (CLOSE, 0, 2),
    (FF_BWD, 5),
    (RS_FINISH, 0),
    (RS_DRAIN, 0),
    (FF_BWD, 4),
    (RS, 4, 1),
    (CLOSE, 0, 1),
    (CLOSE, 0, 0),
    (RS, 2, 3),
    (MERGE, 0, 0, 0),
    (RS, 5, 1),
    (MERGE, 0, 0, 1),
    (CLOSE, 1, 3),
    (RS, 4, 2),
    (MERGE, 0, 1, 0),
    (RS, 3, 3),
    (CLOSE, 1, 2),
    (CLOSE, 1, 1),
    (MERGE, 0, 1, 1),
    (CLOSE, 1, 0),
    (MERGE, 1, 0, 0),
    (SV, 0),
    (RS, 5, 2),
    (RS_FINISH, 2),
    (SV, 1),
    (RS, 4, 3),
    (MERGE, 1, 0, 1),
    (RS, 5, 3),
    (RS_FINISH, 3),
    (MERGE, 1, 1, 0),
    (MERGE, 1, 1, 1),
    (RS_FINISH, 4),
    (SV, 2),
    (SV, 3),
    (RS_FINISH, 5),
    (SV, 4),
    (SV, 5),
)


def make_schedule(groups):
    last = groups - 1
    spans = {1: (1,), 2: range(2, last), 3: range(max(2, last), groups)}
    rounds = (groups * TP).bit_length() - 1
    small = {0: (0,), 1: (1,), 2: (2,), 3: range(3, rounds), 4: (rounds,), 5: (rounds + 1,)}
    plan = []
    for step in PLAN:
        if step[0] in (AG, RS):
            plan += [step[:2] + (s,) for s in spans[step[2]]]
        elif step[0] in (PK, SV):
            plan += [(step[0], n) for n in small[step[1]]]
        else:
            plan.append(step)
    return plan


def main_kernel(cfg, *refs):
    groups, part, depth, width, tokens, length, feeds, back, hidden, bias_cols = cfg
    blocks = feeds + 2
    feed_of = {b: i for i, b in enumerate([0, 1] + list(range(4, blocks)))}
    dp_size = groups * TP
    rounds = dp_size.bit_length() - 1
    (
        x_in,
        cot_in,
        w_query,
        w_key,
        w_value,
        dense_t,
        w_up,
        down_t,
        seg_in,
        freq_in,
        pack_in,
        x_all,
        w_all,
        g_query,
        g_key,
        g_value,
        g_dense,
        g_up,
        g_down,
        pack,
        mine_out,
        other_out,
        sums_out,
        from_left,
        from_right,
        core_in,
        cross_in,
        big,
        wv,
        own,
        fin,
        fin_t,
        ld,
        xs,
        act_v,
        ga_v,
        table,
        norms,
        bias,
        sv,
        sv_in,
        a2a_s,
        a2a_r,
        tok_s,
        tok_r,
        ag_s,
        ag_r,
        rs_s,
        rs_r,
        bk_s,
        bk_r,
        bk_l,
        pk_s,
        pk_r,
        sv_s,
        sv_r,
        cl_s,
        cl_r,
        cr_s,
        cr_r,
        ty_s,
        ty_r,
        ke_s,
        loc,
        stage,
    ) = refs
    dp, ty = lax.axis_index("dp"), lax.axis_index("tensor")
    rank, z = lax.rem(dp, TP), lax.div(dp, TP)
    half_rows = length // 2
    chunk = half_rows // 2

    def remote(src, dst, ssem, rsem, target, tensor=None):
        return pltpu.make_async_remote_copy(
            src_ref=src,
            dst_ref=dst,
            send_sem=ssem,
            recv_sem=rsem,
            device_id=(target, ty if tensor is None else tensor),
            device_id_type=MESH,
        )

    peer = [dp] + [lax.bitwise_xor(dp, k) for k in range(1, TP)]
    prank = [rank] + [lax.bitwise_xor(rank, k) for k in range(1, TP)]
    step_of = (TP, -TP)

    def neighbour(way):
        return lax.rem(dp + step_of[way] + dp_size, dp_size)

    def local(src, dst, sem):
        return pltpu.make_async_copy(src, dst, sem)

    def sources(b):
        if b == 2:
            return ((w_query, HD, 0), (w_key, HD, 0))
        if b == 3:
            return ((w_value, HD, 0), (dense_t, HD, 0))
        i = feed_of[b]
        return ((w_up, hidden, i * HD), (down_t, hidden, i * HD))

    def a2a_copy(b, k, half):
        array, size, offset = sources(b)[half]
        cols = pl.ds(pl.multiple_of(prank[k] * size + offset, LANES), HD)
        rows = pl.ds(pl.multiple_of(z * part + rank * depth, depth), depth)
        dst = w_all.at[b, rows, pl.ds(half * HD, HD)]
        if k == 0:
            return local(array.at[:, cols], dst, a2a_r.at[b])
        return remote(array.at[:, cols], dst, a2a_s.at[b], a2a_r.at[b], peer[k])

    def a2a_start(b):
        for k in (2, 3, 1, 0):
            for half in range(2):
                a2a_copy(b, k, half).start()

    def a2a_wait(b):
        rows = w_all.at[b, pl.ds(pl.multiple_of(z * part, part), part), :]
        local(rows, rows, a2a_r.at[b]).wait()

    def a2a_sent(b):
        rows = w_all.at[b, pl.ds(0, (TP - 1) * depth), :]
        local(rows, rows, a2a_s.at[b]).wait()

    def tok_at(which, k):
        return x_all.at[k] if which == 0 else big.at[2, pl.ds(k * length, length), :]

    def tok_rows(ref, tensor, c):
        return ref.at[pl.ds(pl.multiple_of(tensor * half_rows + c * chunk, chunk), chunk), :]

    def tok_own(which):
        src = (x_in, cot_in)[which]
        return local(src, tok_at(which, 0), tok_r.at[which, 0])

    def tok_beside(which):
        src = (x_in, cot_in)[which]
        return remote(src, tok_at(which, 1), tok_s.at[which, 1], tok_r.at[which, 1], peer[1])

    def tok_cross(which, c):
        src = (x_in, cot_in)[which]
        return remote(
            tok_rows(src, ty, c),
            tok_rows(tok_at(which, 2), ty, c),
            tok_s.at[which, 2 + c],
            tok_r.at[which, 2 + c],
            peer[2],
        )

    def tok_tensor(which, c, receiving=False):
        rows = tok_rows(tok_at(which, 2), 1 - ty if receiving else ty, c)
        return remote(
            rows, rows, tok_s.at[which, 4 + c], tok_r.at[which, 4 + c], dp, tensor=1 - ty
        )

    def tok_last(which):
        return remote(
            tok_at(which, 2), tok_at(which, 3), tok_s.at[which, 6], tok_r.at[which, 6], peer[1]
        )

    def tok_start(which):
        for c in range(2):
            tok_cross(which, c).start()
        tok_beside(which).start()
        tok_own(which).start()

    def tok_y(which, c):
        tok_cross(which, c).wait_recv()
        tok_tensor(which, c).start()

    def tok_core(which):
        for c in range(2):
            tok_tensor(which, c, True).wait_recv()
        tok_last(which).start()

    def tok_sent(which):
        for c in range(2):
            tok_tensor(which, c).wait_send()
        tok_last(which).wait_send()

    def tok_wait(which, k):
        if k == 0:
            tok_own(which).wait()
        elif k == 1:
            tok_beside(which).wait_recv()
        else:
            tok_last(which).wait_recv()

    def tab_copy(hop):
        at = lambda k: table.at[pl.ds(k * length, length), :]
        if hop == 3:
            return remote(at(2), at(3), tok_s.at[2, 3], tok_r.at[2, 3], peer[1])
        return remote(at(0), at(hop), tok_s.at[2, hop], tok_r.at[2, hop], peer[hop])

    def tab_make():
        seg = seg_in[...].astype(F32)
        starts = jnp.zeros(seg.shape, F32)
        for value in range(1, 4):
            before = jnp.sum((seg < value).astype(F32), axis=1, keepdims=True)
            starts = jnp.where(seg == value, before, starts)
        start = jnp.broadcast_to(starts, (8, length)).T[:, 0:1]
        shape = (length, LANES)
        place = lax.broadcasted_iota(jnp.int32, shape, 0).astype(F32)
        lane = lax.broadcasted_iota(jnp.int32, shape, 1)
        angles = (place - start) * freq_in[...]
        sines = jnp.where(lane < ROT, jnp.sin(angles), start)
        table[0:length, :] = jnp.where(lane < ROT // 2, jnp.cos(angles), sines)

    def tab_start():
        for hop in (2, 1):
            tab_copy(hop).start()

    def tab_core():
        tab_copy(2).wait_recv()
        tab_copy(3).start()

    def tab_wait():
        tab_copy(1).wait_recv()
        tab_copy(3).wait_recv()

    def pk_copy(n, receiving=False):
        count = 1 << n
        other = lax.bitwise_xor(dp, count)
        first = lax.div(other if receiving else dp, count) * count
        at = pack.at[pl.ds(first, count)]
        return remote(at, at, pk_s.at[n], pk_r.at[n], other)

    def pk(n):
        if n == 0:
            copy = local(pack_in, pack.at[dp], loc.at[0])
            copy.start()
            copy.wait()
        else:
            pk_copy(n - 1, True).wait_recv()
        pk_copy(n).start()

    def pk_norm():
        pk_copy(rounds - 1, True).wait_recv()
        for j in range(dp_size):
            norms[0:4, j * depth : (j + 1) * depth] = pack[j, 0:4, 0:depth]

    def pk_bias():
        for j in range(dp_size):
            lanes = lambda i: pl.ds(i * HD + j * bias_cols, bias_cols)
            for i in range(3):
                bias[0:1, lanes(i)] = pack[j, pl.ds(8 + 4 * i + rank, 1), 0:bias_cols]
            for i in range(feeds):
                bias[0:1, lanes(3 + i)] = pack[j, pl.ds(20 + feeds * rank + i, 1), 0:bias_cols]

    def x_load(k, h, buffer):
        src = x_in if k == 0 else x_all.at[k]
        rows = pl.ds(pl.multiple_of(h * TILE, TILE), TILE)
        return local(src.at[rows, :], xs.at[buffer], loc.at[buffer])

    def norm_slot(k):
        rows = min(64, TILE)
        x_load(k, 0, 0).start()
        for h in range(length // TILE):
            x_load(k, h, h % 2).wait()
            if (h + 1) * TILE < length:
                x_load(k, h + 1, (h + 1) % 2).start()

            def body(i, carry):
                at = pl.ds(pl.multiple_of(i * rows, rows), rows)
                hat, _ = normed_hat(xs[h % 2, at, :].astype(F32))
                to = pl.ds(pl.multiple_of(k * length + h * TILE + i * rows, rows), rows)
                big[0, to, :] = (hat * norms[0:1, :] + norms[1:2, :]).astype(BF)
                big[1, to, :] = (hat * norms[2:3, :] + norms[3:4, :]).astype(BF)
                return carry

            lax.fori_loop(0, TILE // rows, body, 0)

    def ag_copy(b, s, way, g):
        at = w_all.at[b, pl.ds(pl.multiple_of(g * part, part), part), :]
        return remote(at, at, ag_s.at[b, s - 1, way], ag_r.at[b, s - 1, way], neighbour(way))

    def ag_conditions(s):
        return ((z >= s - 1) & (z <= groups - 2), (z <= groups - s) & (z >= 1))

    def ag_step(b, s):
        go = ag_conditions(s)
        for way in range(2):
            g = (z - s + 1, z + s - 1)[way]

            @pl.when(go[way])
            def _():
                if s > 1:
                    ag_copy(b, s - 1, way, g).wait_recv()
                ag_copy(b, s, way, g).start()

    def ag_finish(b):
        @pl.when(z == groups - 1)
        def _():
            for s in range(1, groups):
                ag_copy(b, s, 0, z - s).wait_recv()

        @pl.when(z == 0)
        def _():
            for s in range(1, groups):
                ag_copy(b, s, 1, z + s).wait_recv()

    def ag_drain(b):
        for s in range(1, groups):
            go = ag_conditions(s)
            for way in range(2):
                g = (z - s + 1, z + s - 1)[way]
                pl.when(go[way])(lambda: ag_copy(b, s, way, g).wait_send())

    def rs_copy(b, t, way, d):
        land = (from_left, from_right)[way]
        return remote(
            own.at[b % OWN_SLOTS, d],
            land.at[b, t - 1],
            rs_s.at[b, t - 1, way],
            rs_r.at[b, t - 1, way],
            neighbour(way),
        )

    rows_add = min(32, BC)

    def rs_load(b, t, way):
        return local((from_left, from_right)[way].at[b, t - 1], ld.at[way], loc.at[4 + way])

    def add_in(b, d, way):
        slot = b % OWN_SLOTS

        def body(i, carry):
            at = pl.ds(pl.multiple_of(i * rows_add, rows_add), rows_add)
            total = own[slot, d, at, :].astype(F32) + ld[way, at, :].astype(F32)
            own[slot, d, at, :] = total.astype(BF)
            return carry

        lax.fori_loop(0, BC // rows_add, body, 0)

    def rs_conditions(t):
        return (z <= t - 1, z >= groups - t)

    def rs_step(b, t):
        go = rs_conditions(t)
        ends = (z == 0, z == groups - 1)
        dest = (z + groups - t, z - groups + t)
        for way in range(2):
            d = dest[way]
            if t > 1:

                @pl.when(go[way] & jnp.logical_not(ends[way]))
                def _():
                    rs_copy(b, t - 1, way, d).wait_recv()
                    rs_load(b, t - 1, way).start()

        for way in range(2):
            d = dest[way]
            if t > 1:

                @pl.when(go[way] & jnp.logical_not(ends[way]))
                def _():
                    rs_load(b, t - 1, way).wait()
                    add_in(b, d, way)

            @pl.when(go[way])
            def _():
                rs_copy(b, t, way, d).start()

    def rs_drain(b):
        for t in range(1, groups):
            go = rs_conditions(t)
            for way in range(2):
                d = (z + groups - t, z - groups + t)[way]
                pl.when(go[way])(lambda: rs_copy(b, t, way, d).wait_send())

    def results(b, half):
        if b == 2:
            return ((g_query, g_key)[half], HD, 0, True)
        if b == 3:
            return ((g_value, g_dense)[half], HD, 0, half == 0)
        return ((g_up, g_down)[half], hidden, feed_of[b] * HD, half == 0)

    def bk_copy(b, k, half):
        array, size, offset, turned = results(b, half)
        at = pl.ds(pl.multiple_of(rank * size + offset, LANES), HD)
        if turned:
            rows = pl.ds(pl.multiple_of(prank[k] * depth, depth), depth)
            src, dst = fin_t.at[b % 2, half, rows, :], array.at[:, at]
        else:
            src, dst = fin.at[b % 2], array.at[at, :]
            if back != part:
                src = src.at[:, pl.ds(pl.multiple_of(prank[k] * depth, LANES), depth)]
        if k == 0:
            return local(src, dst, bk_l.at[b % 2, half])
        return remote(src, dst, bk_s.at[b % 2, k - 1, half], bk_r.at[b], peer[k])

    def bk_arrived(b):
        lanes = sum(depth if results(b, half)[3] else back for half in range(2))
        rows = w_all.at[b, pl.ds(0, (TP - 1) * lanes * HD // BC), :]
        local(rows, rows, bk_r.at[b]).wait()

    def bk_drain(b):
        for half in range(2):
            bk_copy(b, 0, half).wait()
            for k in range(1, TP):
                bk_copy(b, k, half).wait_send()

    def rs_finish(b):
        last = groups - 1
        inner = (z > 0, z < groups - 1)
        for way in range(2):

            @pl.when(inner[way])
            def _():
                rs_copy(b, last, way, z).wait_recv()
                rs_load(b, last, way).start()

        if b >= 2:
            bk_drain(b - 2)
        for way in range(2):
            pl.when(inner[way])(lambda: rs_load(b, last, way).wait())

        slot = b % OWN_SLOTS
        for half in range(2):
            turned = results(b, half)[3]

            def body(i, carry):
                unit = pl.multiple_of(i * LANES, LANES)
                at = pl.ds(half * HD + unit, LANES)
                total = own[slot, z, at, :].astype(F32)
                for way in range(2):
                    total += jnp.where(inner[way], ld[way, at, :].astype(F32), 0.0)
                if turned:
                    fin_t[b % 2, half, :, pl.ds(unit, LANES)] = total.T.astype(BF)
                else:
                    fin[b % 2, pl.ds(unit, LANES), :] = total.astype(BF)
                return carry

            lax.fori_loop(0, HD // LANES, body, 0)
        for k in (2, 3, 1, 0):
            for half in range(2):
                bk_copy(b, k, half).start()

    slot_qk, slot_vd = 2, 0
    slot_of = {0: 0, 1: 1, 2: slot_qk, 3: slot_vd, 4: 1, 5: 1}

    def w_load(b):
        return local(w_all.at[b], wv.at[slot_of[b]], loc.at[6 + slot_of[b]])

    def feed_forward(b):
        i = feed_of[b]
        slot = slot_of[b]
        lanes = slice(i * HD, (i + 1) * HD)

        def body(n, carry):
            at = pl.ds(pl.multiple_of(n * length, length), length)
            pre = dot_nn(big[1, at, :], wv[slot, :, :HD]) + bias[0:1, (3 + i) * HD : (4 + i) * HD]
            grad_act = dot_nn(big[2, at, :], wv[slot, :, HD:])
            cdf = 0.5 * (1.0 + lax.erf(pre * 0.7071067811865476))
            pdf = jnp.exp(-0.5 * pre * pre) * 0.3989422804014327
            act_v[0, at, lanes] = (pre * cdf).astype(BF)
            grad_pre = (grad_act * (cdf + pre * pdf)).astype(BF)
            act_v[1, at, lanes] = grad_pre
            return carry + jnp.sum(grad_pre.astype(F32), axis=0, keepdims=True)

        total = lax.fori_loop(0, TP, body, jnp.zeros((1, HD), F32))
        sv[0, pl.ds(8 + rank, 1), (3 + i) * HD : (4 + i) * HD] = total

    def feed_backward(b):
        slot = b % OWN_SLOTS
        i = feed_of[b]
        lanes = slice(i * HD, (i + 1) * HD)

        def body(d, carry):
            cols = pl.ds(pl.multiple_of(d * part, part), part)
            own[slot, d, :HD, :] = dot_tn(act_v[1, :, lanes], big[1, :, cols]).astype(BF)
            own[slot, d, HD:, :] = dot_tn(act_v[0, :, lanes], big[2, :, cols]).astype(BF)
            return carry

        lax.fori_loop(0, groups, body, 0)

    def attention(between):
        def body(n, carry):
            at = pl.ds(pl.multiple_of(n * length, length), length)
            grads = attend(
                big[0, at, :],
                big[2, at, :],
                wv.at[slot_qk],
                wv.at[slot_vd],
                bias[0:1, : 3 * HD],
                table[at, :],
            )
            for j, g in enumerate(grads):
                ga_v[at, j * HD : (j + 1) * HD] = g
            sums = [jnp.sum(g.astype(F32), axis=0, keepdims=True) for g in grads[:3]]
            carry = carry + jnp.concatenate(sums, axis=1)
            for j, some in enumerate(between):
                if some:

                    @pl.when(n == j)
                    def _():
                        for step in some:
                            run(step)

            return carry

        total = lax.fori_loop(0, TP, body, jnp.zeros((1, 3 * HD), F32))
        sv[0, pl.ds(8 + rank, 1), : 3 * HD] = total

    def attention_back(b):
        slot = b % OWN_SLOTS

        def body(d, carry):
            cols = pl.ds(pl.multiple_of(d * part, part), part)
            if b == 2:
                own[slot, d, :HD, :] = dot_tn(ga_v[:, :HD], big[0, :, cols]).astype(BF)
                own[slot, d, HD:, :] = dot_tn(ga_v[:, HD:BC], big[0, :, cols]).astype(BF)
            else:
                own[slot, d, :HD, :] = dot_tn(ga_v[:, BC : 3 * HD], big[0, :, cols]).astype(BF)
                own[slot, d, HD:, :] = dot_tn(ga_v[:, 3 * HD :], big[2, :, cols]).astype(BF)
            return carry

        lax.fori_loop(0, groups, body, 0)

    def bias_sum():
        rows = min(64, length)

        def body(i, carry):
            at = pl.ds(pl.multiple_of(i * rows, rows), rows)
            return carry + jnp.sum(big[2, at, :].astype(F32), axis=0, keepdims=True)

        total = lax.fori_loop(0, length // rows, body, jnp.zeros((1, width), F32))
        sv[0, 4:5, :] = total * 0.5

    def close_weights(b, half):
        i = feed_of[b]
        lanes = pl.ds((feeds if half == 0 else 0) * HD + i * HD, HD)
        return local(
            w_all.at[b, :, pl.ds(half * HD, HD)], big.at[0, :, lanes], loc.at[9 + 2 * i + half]
        )

    def close_load(b):
        for half in range(2):
            close_weights(b, half).start()

    def close_ready(half):
        for b in feed_of:
            close_weights(b, half).wait()

    sub = TILE // 2

    def staged(q, k, row, count):
        if q == 0 and k == 2:
            return stage.at[pl.ds(pl.multiple_of(row, count), count), :]
        return big.at[1 + q, pl.ds(pl.multiple_of(k * length + row, count), count), :]

    span = min(BC, width)

    def staged_part(q, k, h, i):
        if q == 0 and k == 3:
            rows = pl.ds(pl.multiple_of(i * length + h * TILE, TILE), TILE)
            return wv.at[slot_of[blocks - 1], rows, pl.ds(0, span)]
        cols = pl.ds(pl.multiple_of(i * span, span), span)
        return staged(q, k, h * TILE, TILE).at[:, cols]

    def close_copy(q, k, h, i):
        rows = pl.ds(pl.multiple_of(h * TILE, TILE), TILE)
        return remote(
            staged_part(q, k, h, i),
            core_in.at[q, k // 2, rows, pl.ds(i * span, span)],
            cl_s.at[q, k // 2, h],
            cl_r.at[q, k // 2, h],
            peer[1],
        )

    def close_tile(q, k, h, sem):
        rows = pl.ds(pl.multiple_of(h * TILE, TILE), TILE)
        at = core_in.at[q, k // 2, rows, :]
        return local(at, at, sem.at[q, k // 2, h])

    spans = range(width // span)

    def cross_copy(q, h, c):
        rows = pl.ds(pl.multiple_of(h * TILE + c * sub, sub), sub)
        return remote(
            staged(q, 2, h * TILE + c * sub, sub),
            cross_in.at[q, rows, :],
            cr_s.at[q, h, c],
            cr_r.at[q, h, c],
            peer[2],
        )

    def tensor_copy(q, h, c):
        rows = pl.ds(pl.multiple_of(h * TILE + c * sub, sub), sub)
        return remote(
            staged(q, 0, h * TILE + c * sub, sub),
            other_out.at[q, rows, :],
            ty_s.at[q, h, c],
            ty_r.at[q, h, c],
            dp,
            tensor=1 - ty,
        )

    def keep_copy(q, h, c):
        rows = pl.ds(pl.multiple_of(h * TILE + c * sub, sub), sub)
        return local(staged(q, 0, h * TILE + c * sub, sub), mine_out.at[q, rows, :], ke_s.at[q, h, c])

    def merge(q, h, c):
        cross_copy(q, h, c).wait_recv()
        rows = pl.ds(h * TILE + c * sub, sub)
        copy = local(cross_in.at[q, rows, :], xs.at[1, pl.ds(0, sub), :], loc.at[1])
        copy.start()
        copy.wait()
        rows_here = min(32, sub)
        mine = staged(q, 0, h * TILE + c * sub, sub)

        def body(i, carry):
            at = pl.ds(pl.multiple_of(i * rows_here, rows_here), rows_here)
            mine[at, :] = (mine[at, :].astype(F32) + xs[1, at, :].astype(F32)).astype(BF)
            return carry

        lax.fori_loop(0, sub // rows_here, body, 0)
        tensor_copy(q, h, c).start()
        keep_copy(q, h, c).start()

    ready = []

    def close(q, k):
        if q not in ready:
            ready.append(q)
            close_ready(1 - q)
            if q == 1:
                tok_sent(1)
        col = lambda v: jnp.sum(v, axis=0, keepdims=True)

        def tile(h, carry):
            at = pl.ds(pl.multiple_of(k * length + h * TILE, TILE), TILE)
            if q == 1:
                x_load(k, h, 0).start()
            if k in (0, 2):
                close_tile(q, k + 1, h, cl_r).wait()
                rows = pl.ds(pl.multiple_of(h * TILE, TILE), TILE)
                copy = local(core_in.at[q, k // 2, rows, :], xs.at[1], loc.at[1])
                copy.start()
            if q == 1:
                x_load(k, h, 0).wait()
                x = xs[0].astype(F32)
                mean = jnp.mean(x, axis=-1, keepdims=True)
                inverse = lax.rsqrt(jnp.mean(jnp.square(x - mean), axis=-1, keepdims=True) + 1e-05)
            if k in (0, 2):
                copy.wait()

            def body(i, carry):
                cols = pl.ds(pl.multiple_of(i * span, span), span)
                if q == 0:
                    total = dot_nt(act_v[0, at, :], big[0, cols, : feeds * HD])
                    total += dot_nt(ga_v[at, 3 * HD :], wv[slot_vd, cols, HD:])
                else:
                    hat = (xs[0, :, cols].astype(F32) - mean) * inverse
                    grad_f = dot_nt(act_v[1, at, :], big[0, cols, feeds * HD :])
                    sv[0, 2:3, cols] += col(grad_f * hat)
                    sv[0, 3:4, cols] += col(grad_f)
                    grad_a = dot_nt(ga_v[at, :BC], wv[slot_qk, cols, :])
                    grad_a += dot_nt(ga_v[at, BC : 3 * HD], wv[slot_vd, cols, :HD])
                    sv[0, 0:1, cols] += col(grad_a * hat)
                    sv[0, 1:2, cols] += col(grad_a)
                    total = grad_f * norms[2:3, cols] + grad_a * norms[0:1, cols]
                if k in (0, 2):
                    total += xs[1, :, cols].astype(F32)
                staged_part(q, k, h, i)[...] = total.astype(BF)
                return carry

            lax.fori_loop(0, width // span, body, 0)
            if k in (1, 3):
                for i in spans:
                    close_copy(q, k, h, i).start()
            if k == 2:
                for c in range(2):
                    cross_copy(q, h, c).start()
            return carry

        lax.fori_loop(0, length // TILE, tile, 0)

    def sv_copy(n):
        if n < rounds:
            return remote(
                sv.at[n], sv_in.at[n], sv_s.at[n], sv_r.at[n], lax.bitwise_xor(dp, 1 << n)
            )
        rows = pl.ds(0, 8)
        return remote(
            sv.at[n, rows], sv_in.at[n, rows], sv_s.at[n], sv_r.at[n], dp, tensor=1 - ty
        )

    def sv_step(n):
        if n > 0:
            sv_copy(n - 1).wait_recv()
        if n <= rounds:
            if n > 0:
                sv[n] = sv[n - 1] + sv_in[n - 1]
            sv_copy(n).start()
        else:
            sums_out[0:8] = sv[rounds, 0:8] + sv_in[rounds, 0:8]
            sums_out[8:16] = sv[rounds, 8:16]

    barrier = pltpu.get_barrier_semaphore()

    def greet(target, tensor):
        pl.semaphore_signal(barrier, inc=1, device_id=(target, tensor), device_id_type=MESH)

    greet(dp, 1 - ty)
    for k in range(1, TP):
        greet(peer[k], ty)
    bit = TP
    while bit < dp_size:
        greet(lax.bitwise_xor(dp, bit), ty)
        bit *= 2
    odd = lax.rem(z, 2) == 1
    up_more, down_more = odd & (z < groups - 1), jnp.logical_not(odd) & (z > 0)
    pl.when(up_more)(lambda: greet(neighbour(0), ty))
    pl.when(down_more)(lambda: greet(neighbour(1), ty))
    count = rounds + 2
    more = up_more | down_more
    pl.when(more)(lambda: pl.semaphore_wait(barrier, count + 1))
    pl.when(jnp.logical_not(more))(lambda: pl.semaphore_wait(barrier, count))

    steps = {
        A2A_START: a2a_start,
        A2A_WAIT: a2a_wait,
        TOK_START: tok_start,
        TOK_Y: tok_y,
        TOK_CORE: tok_core,
        TOK_WAIT: tok_wait,
        TAB_MAKE: tab_make,
        TAB_START: tab_start,
        TAB_CORE: tab_core,
        TAB_WAIT: tab_wait,
        PK: pk,
        PK_NORM: pk_norm,
        PK_BIAS: pk_bias,
        NORM: norm_slot,
        AG: ag_step,
        AG_FINISH: ag_finish,
        LOAD: lambda b: w_load(b).start(),
        LOAD_WAIT: lambda b: w_load(b).wait(),
        FF_FWD: feed_forward,
        FF_BWD: feed_backward,
        ATTN_BWD: attention_back,
        BIAS_SUM: bias_sum,
        RS: rs_step,
        RS_FINISH: rs_finish,
        RS_DRAIN: rs_drain,
        CLOSE_LOAD: close_load,
        CLOSE: close,
        MERGE: merge,
        SV: sv_step,
    }

    def run(step):
        steps[step[0]](*step[1:])

    sv[0] = jnp.zeros(sv.shape[1:], F32)
    ld[...] = jnp.zeros(ld.shape, BF)
    plan = make_schedule(groups)
    plan.insert(0, (TAB_MAKE,))
    rows_at = [plan.index((ATTN_ROW, n)) for n in range(TP)]
    for step in plan[: rows_at[0]]:
        run(step)
    attention([plan[i + 1 : j] for i, j in zip(rows_at, rows_at[1:])] + [[]])
    for step in plan[rows_at[-1] + 1 :]:
        run(step)

    drained = [step[1] for step in plan if step[0] == RS_DRAIN]
    for b in range(blocks):
        a2a_sent(b)
        ag_drain(b)
        if b not in drained:
            rs_drain(b)
    tok_own(0).wait()
    for which in range(2):
        tok_beside(which).wait_send()
        for c in range(2):
            tok_cross(which, c).wait_send()
    tok_sent(0)
    for hop in (1, 2, 3):
        tab_copy(hop).wait_send()
    for n in range(rounds):
        pk_copy(n).wait_send()
    for n in range(rounds + 1):
        sv_copy(n).wait_send()
    for q in range(2):
        for h in range(length // TILE):
            for k in (1, 3):
                close_tile(q, k, h, cl_s).wait()
            for c in range(2):
                cross_copy(q, h, c).wait_send()
                tensor_copy(q, h, c).wait_send()
                tensor_copy(q, h, c).wait_recv()
                keep_copy(q, h, c).wait()
    bk_drain(blocks - 2)
    bk_drain(blocks - 1)
    for b in range(blocks):
        bk_arrived(b)


def run_main(groups, x, cot, weights, segments, pack, bias_cols):
    length, width = x.shape
    depth = weights[0].shape[0]
    part = width // groups
    tokens = TP * length
    hidden = weights[4].shape[1] // TP
    feeds = hidden // HD
    blocks = feeds + 2
    dp_size = groups * TP
    rounds = dp_size.bit_length() - 1
    back = depth if depth % LANES == 0 else part
    cfg = (groups, part, depth, width, tokens, length, feeds, back, hidden, bias_cols)
    hbm = pl.BlockSpec(memory_space=pltpu.HBM)
    vmem = pl.BlockSpec(memory_space=pltpu.VMEM)
    sem = pltpu.SemaphoreType.DMA
    shape = jax.ShapeDtypeStruct
    tiles = length // TILE
    steps_in = (jnp.arange(LANES) % (ROT // 2)).astype(F32)
    freq = (10000.0 ** (-2.0 * steps_in / ROT)).reshape(1, LANES)
    return pl.pallas_call(
        functools.partial(main_kernel, cfg),
        out_shape=(
            shape((TP, length, width), BF),
            shape((blocks, width, BC), BF),
            shape((depth, TP * HD), BF),
            shape((depth, TP * HD), BF),
            shape((depth, TP * HD), BF),
            shape((TP * HD, back), BF),
            shape((depth, TP * hidden), BF),
            shape((TP * hidden, back), BF),
            shape((dp_size,) + pack.shape, F32),
            shape((2, length, width), BF),
            shape((2, length, width), BF),
            shape((16, width), F32),
            shape((blocks, groups, BC, part), BF),
            shape((blocks, groups, BC, part), BF),
            shape((2, 2, length, width), BF),
            shape((2, length, width), BF),
        ),
        in_specs=[hbm] * 8 + [vmem] * 2 + [hbm],
        out_specs=(hbm,) * 8 + (vmem,) + (hbm,) * 2 + (vmem,) + (hbm,) * 4,
        scratch_shapes=[
            pltpu.VMEM((3, tokens, width), BF),
            pltpu.VMEM((W_SLOTS, width, BC), BF),
            pltpu.VMEM((OWN_SLOTS, groups, BC, part), BF),
            pltpu.VMEM((2, HD, part), BF),
            pltpu.VMEM((2, 2, part, HD), BF),
            pltpu.VMEM((2, BC, part), BF),
            pltpu.VMEM((2, TILE, width), BF),
            pltpu.VMEM((2, tokens, feeds * HD), BF),
            pltpu.VMEM((tokens, 4 * HD), BF),
            pltpu.VMEM((tokens, LANES), F32),
            pltpu.VMEM((8, width), F32),
            pltpu.VMEM((8, (3 + feeds) * HD), F32),
            pltpu.VMEM((rounds + 1, 16, width), F32),
            pltpu.VMEM((rounds + 1, 16, width), F32),
            sem((blocks,)),
            sem((blocks,)),
            sem((3, 7)),
            sem((3, 7)),
            sem((blocks, groups - 1, 2)),
            sem((blocks, groups - 1, 2)),
            sem((blocks, groups - 1, 2)),
            sem((blocks, groups - 1, 2)),
            sem((2, TP - 1, 2)),
            sem((blocks,)),
            sem((2, 2)),
            sem((rounds,)),
            sem((rounds,)),
            sem((rounds + 1,)),
            sem((rounds + 1,)),
            sem((2, 2, tiles)),
            sem((2, 2, tiles)),
            sem((2, tiles, 2)),
            sem((2, tiles, 2)),
            sem((2, tiles, 2)),
            sem((2, tiles, 2)),
            sem((2, tiles, 2)),
            sem((9 + 2 * feeds,)),
            pltpu.VMEM((length, width), BF),
        ],
        compiler_params=pltpu.CompilerParams(
            collective_id=0, has_side_effects=True, vmem_limit_bytes=67043328
        ),
        name="main",
    )(x, cot, *weights, segments, freq, pack)


def finish_kernel(cols, mine, other, x_ref, cot, packs, sums, *refs):
    grads, (hidden, grad_in), made, small, bias = refs[:6], refs[6:8], refs[8:14], refs[14:-1], refs[-1]
    devices = packs.shape[0]
    depth = bias.shape[1] // devices

    @pl.when(pl.program_id(0) == 0)
    def _():
        for j in range(devices):
            bias[0:1, j * depth : (j + 1) * depth] = packs[j, 4:5, :depth] + packs[j, 5:6, :depth]
        dp = lax.axis_index("dp")
        out_query, out_key, out_value, out_up, out_vectors = small

        def mine_of(lanes):
            wide = pltpu.roll(sums[8 : 8 + 8, lanes], lax.rem(HD - dp * cols, HD), 1)
            return wide[:TP, :cols]

        out_query[...] = mine_of(slice(0, HD))
        out_key[...] = sums[8 : 8 + TP, HD : HD + ROT]
        out_value[...] = mine_of(slice(2 * HD, 3 * HD))
        units = out_up.shape[0] // TP
        for i in range(units):
            piece = mine_of(slice((3 + i) * HD, (4 + i) * HD))
            for rank in range(TP):
                row = rank * units + i
                out_up[row : row + 1, :] = piece[rank : rank + 1, :]
        if depth % LANES == 0:
            out_vectors[...] = sums[0:8, pl.ds(pl.multiple_of(dp * depth, LANES), depth)]
        else:
            out_vectors[...] = sums[0:8, :]

    x = x_ref[...].astype(F32)
    hidden[...] = (x + (mine[0].astype(F32) + other[0].astype(F32)) + bias[...]).astype(BF)
    hat, inverse = normed_hat(x)
    h = mine[1].astype(F32) + other[1].astype(F32)
    grad_in[...] = cot[...].astype(F32) + inverse * (
        h
        - jnp.mean(h, axis=-1, keepdims=True)
        - hat * jnp.mean(h * hat, axis=-1, keepdims=True)
    )
    for source, target in zip(grads, made):
        target[...] = source[...].astype(F32)


def finish(mine, other, x, cot, packs, sums, grads, cols):
    length, width = x.shape
    depth = grads[0].shape[0]
    steps = max(1, min(8, depth // 16))
    tile = lambda a: pl.BlockSpec((a.shape[0] // steps, a.shape[1]), lambda i: (i, 0))
    pair = pl.BlockSpec((2, length // steps, width), lambda i: (0, i, 0))
    shape = jax.ShapeDtypeStruct
    units = grads[4].shape[1] // HD
    whole = lambda s: pl.BlockSpec(s, lambda i: (0,) * len(s))
    small = [(TP, cols), (TP, ROT), (TP, cols), (units, cols)]
    small.append((8, depth if depth % LANES == 0 else width))
    return pl.pallas_call(
        functools.partial(finish_kernel, cols),
        grid=(steps,),
        out_shape=(shape(x.shape, BF), shape(x.shape, F32))
        + tuple(shape(g.shape, F32) for g in grads)
        + tuple(shape(s, F32) for s in small),
        in_specs=[pair, pair, tile(x), tile(cot), whole(packs.shape), whole(sums.shape)]
        + [tile(g) for g in grads],
        out_specs=[tile(x), tile(x)] + [tile(g) for g in grads] + [whole(s) for s in small],
        scratch_shapes=[pltpu.VMEM((1, width), F32)],
        compiler_params=pltpu.CompilerParams(vmem_limit_bytes=67043328),
        name="finish",
    )(mine, other, x, cot, packs, sums, *grads)


def make_shards(dp_size):
    groups = dp_size // TP

    def shards(
        hidden_in,
        segments,
        cotangent,
        w_query,
        w_key,
        w_value,
        w_dense,
        w_up,
        w_down,
        bias_query,
        bias_key,
        bias_value,
        bias_dense,
        bias_up,
        bias_down,
        attend_gain,
        attend_shift,
        feed_gain,
        feed_shift,
    ):
        dp = lax.axis_index("dp")
        rank = dp % TP
        length, width = hidden_in.shape
        depth = w_query.shape[0]
        cols = bias_query.shape[1]

        vectors = (attend_gain, attend_shift, feed_gain, feed_shift, bias_dense, bias_down)
        wide = lambda a: jnp.pad(a.astype(F32), ((0, 0), (0, LANES - a.shape[1])))
        pack = jnp.concatenate(
            [wide(jnp.stack(vectors + (vectors[0],) * 2))]
            + [wide(a) for a in (bias_query, bias_key, bias_value, bias_up)],
            axis=0,
        )
        pack = jnp.pad(pack, ((0, -pack.shape[0] % 8), (0, 0)))

        weights = (w_query, w_key, w_value, w_dense.T, w_up, w_down.T)
        made = run_main(groups, hidden_in, cotangent, weights, segments, pack, cols)
        grads, (packs, mine, other, sums) = made[2:8], made[8:12]

        if grads[3].shape[1] != depth:
            mine_of = lambda g: lax.dynamic_slice_in_dim(g, rank * depth, depth, 1)
            grads = grads[:3] + (mine_of(grads[3]), grads[4], mine_of(grads[5]))
        done = finish(mine, other, hidden_in, cotangent, packs, sums, grads, cols)
        out_query, out_key, out_value, out_up, vec = done[8:]
        if vec.shape[1] != depth:
            vec = lax.dynamic_slice_in_dim(vec, dp * depth, depth, 1)
        return done[:8] + (
            out_query,
            out_key,
            out_value,
            vec[4],
            out_up,
            vec[4],
            vec[0],
            vec[1],
            vec[2],
            vec[3],
        )

    return shards


def solution(mesh):
    shards = make_shards(mesh.shape["dp"])
    in_specs = (
        P("dp", None),
        P("dp", None),
        P("dp", None),
        P("dp", "tensor"),
        P("dp", "tensor"),
        P("dp", "tensor"),
        P("tensor", "dp"),
        P("dp", "tensor"),
        P("tensor", "dp"),
        P("tensor", "dp"),
        P("tensor", "dp"),
        P("tensor", "dp"),
        P("dp"),
        P("tensor", "dp"),
        P("dp"),
        P("dp"),
        P("dp"),
        P("dp"),
        P("dp"),
    )
    out_specs = (
        P("dp", None),
        P("dp", None),
        P("dp", "tensor"),
        P("dp", "tensor"),
        P("dp", "tensor"),
        P("tensor", "dp"),
        P("dp", "tensor"),
        P("tensor", "dp"),
        P("tensor", "dp"),
        P("tensor", None),
        P("tensor", "dp"),
        P("dp"),
        P("tensor", "dp"),
        P("dp"),
        P("dp"),
        P("dp"),
        P("dp"),
        P("dp"),
    )
    return jax.shard_map(shards, mesh=mesh, in_specs=in_specs, out_specs=out_specs, check_vma=False)
```

```python
import functools

import jax
import jax.numpy as jnp
from jax import lax
from jax.experimental import pallas as pl
from jax.experimental.pallas import tpu as pltpu
from jax.sharding import PartitionSpec as P

HD = 256
ROT = 64
TP = 4
LANES = 128
BC = 2 * HD
BF = jnp.bfloat16
F32 = jnp.float32
MESH = pl.DeviceIdType.MESH
OWN_SLOTS = 4
W_SLOTS = 3
TILE = 256


def dot_nn(a, b):
    return lax.dot_general(a, b, (((1,), (0,)), ((), ())), preferred_element_type=F32)


def dot_nt(a, b):
    return lax.dot_general(a, b, (((1,), (1,)), ((), ())), preferred_element_type=F32)


def dot_tn(a, b):
    return lax.dot_general(a, b, (((0,), (0,)), ((), ())), preferred_element_type=F32)


def normed_hat(x):
    mean = jnp.mean(x, axis=-1, keepdims=True)
    centred = x - mean
    inverse = lax.rsqrt(jnp.mean(centred * centred, axis=-1, keepdims=True) + 1e-05)
    return centred * inverse, inverse


def swap_halves(u):
    half = ROT // 2
    lane = lax.broadcasted_iota(jnp.int32, u.shape, 1)
    return jnp.where(lane < half, pltpu.roll(u, LANES - half, 1), pltpu.roll(u, half, 1))


def turn(u, cosine, sine):
    head = u[:, :LANES]
    return jnp.concatenate([head * cosine + swap_halves(head) * sine, u[:, LANES:]], axis=1)


def attend(normed, cot, w_qk, w_vd, bias, table):
    scale = HD ** (-0.5)
    tokens = normed.shape[0]
    q = dot_nn(normed, w_qk[:, :HD]) + bias[:, :HD]
    k = dot_nn(normed, w_qk[:, HD:]) + bias[:, HD : 2 * HD]
    v_low = (dot_nn(normed, w_vd[:, :HD]) + bias[:, 2 * HD :]).astype(BF)
    grad_att = dot_nn(cot, w_vd[:, HD:]).astype(BF)
    half = ROT // 2
    lane = lax.broadcasted_iota(jnp.int32, table.shape, 1)
    later, sooner = pltpu.roll(table, half, 1), pltpu.roll(table, LANES - half, 1)
    cosine = jnp.where(lane < half, table, jnp.where(lane < ROT, later, 1.0))
    sine = jnp.where(lane < half, -sooner, jnp.where(lane < ROT, table, 0.0))
    start = table[:, ROT : ROT + 1].astype(jnp.int32)
    q_rot = turn(q, cosine, sine).astype(BF)
    k_rot = turn(k, cosine, sine).astype(BF)
    size = tokens // 2
    attended, grad_q, grad_k, grad_v = [], [], None, None
    for first in range(0, tokens, size):
        end = first + size
        mine = slice(first, end)
        scores = dot_nt(q_rot[mine], k_rot[:end]) * scale
        row = lax.broadcasted_iota(jnp.int32, (size, end), 0) + first
        col = lax.broadcasted_iota(jnp.int32, (size, end), 1)
        allowed = (col <= row) & (col >= start[mine])
        scores = jnp.where(allowed, scores, -1e30)
        top = jnp.max(scores, axis=-1, keepdims=True)
        weights = jnp.exp(scores - top)
        probs = weights / jnp.sum(weights, axis=-1, keepdims=True)
        probs_low = probs.astype(BF)
        attended.append(dot_nn(probs_low, v_low[:end]).astype(BF))
        grad_probs = dot_nt(grad_att[mine], v_low[:end])
        delta = jnp.sum(probs * grad_probs, axis=-1, keepdims=True)
        grad_scores = (probs * (grad_probs - delta)).astype(BF)
        grad_q.append(dot_nn(grad_scores, k_rot[:end]))
        more_k, more_v = dot_tn(grad_scores, q_rot[mine]), dot_tn(probs_low, grad_att[mine])
        if grad_k is not None:
            more_k = jnp.concatenate([more_k[:first] + grad_k, more_k[first:]], axis=0)
            more_v = jnp.concatenate([more_v[:first] + grad_v, more_v[first:]], axis=0)
        grad_k, grad_v = more_k, more_v
    grad_q = jnp.concatenate(grad_q, axis=0)
    grad_q = turn(grad_q * scale, cosine, -sine).astype(BF)
    grad_k = turn(grad_k * scale, cosine, -sine).astype(BF)
    return grad_q, grad_k, grad_v.astype(BF), jnp.concatenate(attended, axis=0)


(
    A2A_START,
    A2A_WAIT,
    TOK_START,
    TOK_Y,
    TOK_CORE,
    TOK_WAIT,
    TAB_MAKE,
    TAB_START,
    TAB_CORE,
    TAB_WAIT,
    PK,
    PK_NORM,
    PK_BIAS,
    NORM,
    AG,
    AG_FINISH,
    LOAD,
    LOAD_WAIT,
    FF_FWD,
    FF_BWD,
    ATTN_ROW,
    ATTN_BWD,
    BIAS_SUM,
    RS,
    RS_FINISH,
    RS_DRAIN,
    CLOSE_LOAD,
    CLOSE,
    MERGE,
    SV,
) = range(30)

PLAN = (
    (A2A_START, 1),
    (A2A_START, 0),
    (A2A_START, 3),
    (A2A_WAIT, 1),
    (AG, 1, 1),
    (PK, 0),
    (A2A_WAIT, 3),
    (A2A_WAIT, 0),
    (AG, 0, 1),
    (PK, 1),
    (A2A_START, 4),
    (PK, 2),
    (TOK_START, 0),
    (AG, 1, 2),
    (PK, 3),
    (TOK_START, 1),
    (AG, 1, 3),
    (A2A_START, 2),
    (AG, 3, 1),
    (TOK_Y, 0, 0),
    (TOK_WAIT, 0, 1),
    (AG_FINISH, 1),
    (TOK_WAIT, 1, 1),
    (TOK_Y, 0, 1),
    (PK_NORM,),
    (PK_BIAS,),
    (TOK_WAIT, 1, 0),
    (AG, 3, 2),
    (TOK_CORE, 0),
    (AG, 0, 2),
    (TAB_START,),
    (LOAD, 1),
    (AG, 0, 3),
    (A2A_START, 5),
    (TOK_Y, 1, 0),
    (A2A_WAIT, 2),
    (AG, 2, 1),
    (TOK_WAIT, 0, 3),
    (A2A_WAIT, 4),
    (A2A_WAIT, 5),
    (LOAD_WAIT, 1),
    (TOK_Y, 1, 1),
    (AG, 3, 3),
    (AG, 5, 1),
    (AG, 2, 2),
    (TOK_CORE, 1),
    (AG, 2, 3),
    (AG, 5, 2),
    (AG_FINISH, 0),
    (TAB_CORE,),
    (NORM, 1),
    (NORM, 0),
    (AG, 4, 1),
    (TOK_WAIT, 1, 3),
    (TAB_WAIT,),
    (LOAD, 0),
    (NORM, 2),
    (NORM, 3),
    (FF_FWD, 1),
    (LOAD_WAIT, 0),
    (AG_FINISH, 3),
    (FF_FWD, 0),
    (FF_BWD, 1),
    (RS, 1, 1),
    (AG, 4, 2),
    (FF_BWD, 0),
    (RS, 0, 1),
    (AG_FINISH, 2),
    (RS, 0, 2),
    (LOAD, 3),
    (AG, 4, 3),
    (LOAD, 2),
    (AG, 5, 3),
    (LOAD_WAIT, 2),
    (LOAD_WAIT, 3),
    (RS, 1, 2),
    (ATTN_ROW, 0),
    (ATTN_ROW, 1),
    (ATTN_ROW, 2),
    (ATTN_ROW, 3),
    (ATTN_BWD, 2),
    (RS, 1, 3),
    (RS, 2, 1),
    (ATTN_BWD, 3),
    (AG_FINISH, 4),
    (LOAD, 4),
    (BIAS_SUM,),
    (RS, 3, 1),
    (CLOSE_LOAD, 0),
    (LOAD_WAIT, 4),
    (CLOSE_LOAD, 4),
    (FF_FWD, 4),
    (AG_FINISH, 5),
    (CLOSE_LOAD, 5),
    (CLOSE_LOAD, 1),
    (RS, 0, 3),
    (LOAD, 5),
    (RS, 2, 2),
    (LOAD_WAIT, 5),
    (FF_FWD, 5),
    (RS, 3, 2),
    (CLOSE, 0, 3),
    (RS_FINISH, 1),
    (RS_DRAIN, 1),
    (CLOSE, 0, 2),
    (FF_BWD, 5),
    (RS_FINISH, 0),
    (RS_DRAIN, 0),
    (FF_BWD, 4),
    (RS, 4, 1),
    (CLOSE, 0, 1),
    (CLOSE, 0, 0),
    (RS, 2, 3),
    (MERGE, 0, 0, 0),
    (RS, 5, 1),
    (MERGE, 0, 0, 1),
    (CLOSE, 1, 3),
    (RS, 4, 2),
    (MERGE, 0, 1, 0),
    (RS, 3, 3),
    (CLOSE, 1, 2),
    (CLOSE, 1, 1),
    (MERGE, 0, 1, 1),
    (CLOSE, 1, 0),
    (MERGE, 1, 0, 0),
    (SV, 0),
    (RS, 5, 2),
    (RS_FINISH, 2),
    (SV, 1),
    (RS, 4, 3),
    (MERGE, 1, 0, 1),
    (RS, 5, 3),
    (RS_FINISH, 3),
    (MERGE, 1, 1, 0),
    (MERGE, 1, 1, 1),
    (RS_FINISH, 4),
    (SV, 2),
    (SV, 3),
    (RS_FINISH, 5),
    (SV, 4),
    (SV, 5),
)


def make_schedule(groups):
    last = groups - 1
    spans = {1: (1,), 2: range(2, last), 3: range(max(2, last), groups)}
    rounds = (groups * TP).bit_length() - 1
    small = {0: (0,), 1: (1,), 2: (2,), 3: range(3, rounds), 4: (rounds,), 5: (rounds + 1,)}
    plan = []
    for step in PLAN:
        if step[0] in (AG, RS):
            plan += [step[:2] + (s,) for s in spans[step[2]]]
        elif step[0] in (PK, SV):
            plan += [(step[0], n) for n in small[step[1]]]
        else:
            plan.append(step)
    return plan


def main_kernel(cfg, *refs):
    groups, part, depth, width, tokens, length, feeds, back, hidden, bias_cols = cfg
    blocks = feeds + 2
    feed_of = {b: i for i, b in enumerate([0, 1] + list(range(4, blocks)))}
    dp_size = groups * TP
    rounds = dp_size.bit_length() - 1
    (
        x_in,
        cot_in,
        w_query,
        w_key,
        w_value,
        dense_t,
        w_up,
        down_t,
        seg_in,
        freq_in,
        pack_in,
        x_all,
        w_all,
        g_query,
        g_key,
        g_value,
        g_dense,
        g_up,
        g_down,
        pack,
        mine_out,
        other_out,
        sums_out,
        from_left,
        from_right,
        core_in,
        cross_in,
        big,
        wv,
        own,
        fin,
        fin_t,
        ld,
        xs,
        act_v,
        ga_v,
        table,
        norms,
        bias,
        sv,
        sv_in,
        a2a_s,
        a2a_r,
        tok_s,
        tok_r,
        ag_s,
        ag_r,
        rs_s,
        rs_r,
        bk_s,
        bk_r,
        bk_l,
        pk_s,
        pk_r,
        sv_s,
        sv_r,
        cl_s,
        cl_r,
        cr_s,
        cr_r,
        ty_s,
        ty_r,
        ke_s,
        loc,
        stage,
    ) = refs
    dp, ty = lax.axis_index("dp"), lax.axis_index("tensor")
    rank, z = lax.rem(dp, TP), lax.div(dp, TP)
    half_rows = length // 2
    chunk = half_rows // 2

    def remote(src, dst, ssem, rsem, target, tensor=None):
        return pltpu.make_async_remote_copy(
            src_ref=src,
            dst_ref=dst,
            send_sem=ssem,
            recv_sem=rsem,
            device_id=(target, ty if tensor is None else tensor),
            device_id_type=MESH,
        )

    peer = [dp] + [lax.bitwise_xor(dp, k) for k in range(1, TP)]
    prank = [rank] + [lax.bitwise_xor(rank, k) for k in range(1, TP)]
    step_of = (TP, -TP)

    def neighbour(way):
        return lax.rem(dp + step_of[way] + dp_size, dp_size)

    def local(src, dst, sem):
        return pltpu.make_async_copy(src, dst, sem)

    def sources(b):
        if b == 2:
            return ((w_query, HD, 0), (w_key, HD, 0))
        if b == 3:
            return ((w_value, HD, 0), (dense_t, HD, 0))
        i = feed_of[b]
        return ((w_up, hidden, i * HD), (down_t, hidden, i * HD))

    def a2a_copy(b, k, half):
        array, size, offset = sources(b)[half]
        cols = pl.ds(pl.multiple_of(prank[k] * size + offset, LANES), HD)
        rows = pl.ds(pl.multiple_of(z * part + rank * depth, depth), depth)
        dst = w_all.at[b, rows, pl.ds(half * HD, HD)]
        if k == 0:
            return local(array.at[:, cols], dst, a2a_r.at[b])
        return remote(array.at[:, cols], dst, a2a_s.at[b], a2a_r.at[b], peer[k])

    def a2a_start(b):
        for k in (2, 3, 1, 0):
            for half in range(2):
                a2a_copy(b, k, half).start()

    def a2a_wait(b):
        rows = w_all.at[b, pl.ds(pl.multiple_of(z * part, part), part), :]
        local(rows, rows, a2a_r.at[b]).wait()

    def a2a_sent(b):
        rows = w_all.at[b, pl.ds(0, (TP - 1) * depth), :]
        local(rows, rows, a2a_s.at[b]).wait()

    def tok_at(which, k):
        return x_all.at[k] if which == 0 else big.at[2, pl.ds(k * length, length), :]

    def tok_rows(ref, tensor, c):
        return ref.at[pl.ds(pl.multiple_of(tensor * half_rows + c * chunk, chunk), chunk), :]

    def tok_own(which):
        src = (x_in, cot_in)[which]
        return local(src, tok_at(which, 0), tok_r.at[which, 0])

    def tok_beside(which):
        src = (x_in, cot_in)[which]
        return remote(src, tok_at(which, 1), tok_s.at[which, 1], tok_r.at[which, 1], peer[1])

    def tok_cross(which, c):
        src = (x_in, cot_in)[which]
        return remote(
            tok_rows(src, ty, c),
            tok_rows(tok_at(which, 2), ty, c),
            tok_s.at[which, 2 + c],
            tok_r.at[which, 2 + c],
            peer[2],
        )

    def tok_tensor(which, c, receiving=False):
        rows = tok_rows(tok_at(which, 2), 1 - ty if receiving else ty, c)
        return remote(
            rows, rows, tok_s.at[which, 4 + c], tok_r.at[which, 4 + c], dp, tensor=1 - ty
        )

    def tok_last(which):
        return remote(
            tok_at(which, 2), tok_at(which, 3), tok_s.at[which, 6], tok_r.at[which, 6], peer[1]
        )

    def tok_start(which):
        for c in range(2):
            tok_cross(which, c).start()
        tok_beside(which).start()
        tok_own(which).start()

    def tok_y(which, c):
        tok_cross(which, c).wait_recv()
        tok_tensor(which, c).start()

    def tok_core(which):
        for c in range(2):
            tok_tensor(which, c, True).wait_recv()
        tok_last(which).start()

    def tok_sent(which):
        for c in range(2):
            tok_tensor(which, c).wait_send()
        tok_last(which).wait_send()

    def tok_wait(which, k):
        if k == 0:
            tok_own(which).wait()
        elif k == 1:
            tok_beside(which).wait_recv()
        else:
            tok_last(which).wait_recv()

    def tab_copy(hop):
        at = lambda k: table.at[pl.ds(k * length, length), :]
        if hop == 3:
            return remote(at(2), at(3), tok_s.at[2, 3], tok_r.at[2, 3], peer[1])
        return remote(at(0), at(hop), tok_s.at[2, hop], tok_r.at[2, hop], peer[hop])

    def tab_make():
        seg = seg_in[...].astype(F32)
        starts = jnp.zeros(seg.shape, F32)
        for value in range(1, 4):
            before = jnp.sum((seg < value).astype(F32), axis=1, keepdims=True)
            starts = jnp.where(seg == value, before, starts)
        start = jnp.broadcast_to(starts, (8, length)).T[:, 0:1]
        shape = (length, LANES)
        place = lax.broadcasted_iota(jnp.int32, shape, 0).astype(F32)
        lane = lax.broadcasted_iota(jnp.int32, shape, 1)
        angles = (place - start) * freq_in[...]
        sines = jnp.where(lane < ROT, jnp.sin(angles), start)
        table[0:length, :] = jnp.where(lane < ROT // 2, jnp.cos(angles), sines)

    def tab_start():
        for hop in (2, 1):
            tab_copy(hop).start()

    def tab_core():
        tab_copy(2).wait_recv()
        tab_copy(3).start()

    def tab_wait():
        tab_copy(1).wait_recv()
        tab_copy(3).wait_recv()

    def pk_copy(n, receiving=False):
        count = 1 << n
        other = lax.bitwise_xor(dp, count)
        first = lax.div(other if receiving else dp, count) * count
        at = pack.at[pl.ds(first, count)]
        return remote(at, at, pk_s.at[n], pk_r.at[n], other)

    def pk(n):
        if n == 0:
            copy = local(pack_in, pack.at[dp], loc.at[0])
            copy.start()
            copy.wait()
        else:
            pk_copy(n - 1, True).wait_recv()
        pk_copy(n).start()

    def pk_norm():
        pk_copy(rounds - 1, True).wait_recv()
        for j in range(dp_size):
            norms[0:4, j * depth : (j + 1) * depth] = pack[j, 0:4, 0:depth]

    def pk_bias():
        for j in range(dp_size):
            lanes = lambda i: pl.ds(i * HD + j * bias_cols, bias_cols)
            for i in range(3):
                bias[0:1, lanes(i)] = pack[j, pl.ds(8 + 4 * i + rank, 1), 0:bias_cols]
            for i in range(feeds):
                bias[0:1, lanes(3 + i)] = pack[j, pl.ds(20 + feeds * rank + i, 1), 0:bias_cols]

    def x_load(k, h, buffer):
        src = x_in if k == 0 else x_all.at[k]
        rows = pl.ds(pl.multiple_of(h * TILE, TILE), TILE)
        return local(src.at[rows, :], xs.at[buffer], loc.at[buffer])

    def norm_slot(k):
        rows = min(64, TILE)
        x_load(k, 0, 0).start()
        for h in range(length // TILE):
            x_load(k, h, h % 2).wait()
            if (h + 1) * TILE < length:
                x_load(k, h + 1, (h + 1) % 2).start()

            def body(i, carry):
                at = pl.ds(pl.multiple_of(i * rows, rows), rows)
                hat, _ = normed_hat(xs[h % 2, at, :].astype(F32))
                to = pl.ds(pl.multiple_of(k * length + h * TILE + i * rows, rows), rows)
                big[0, to, :] = (hat * norms[0:1, :] + norms[1:2, :]).astype(BF)
                big[1, to, :] = (hat * norms[2:3, :] + norms[3:4, :]).astype(BF)
                return carry

            lax.fori_loop(0, TILE // rows, body, 0)

    def ag_copy(b, s, way, g):
        at = w_all.at[b, pl.ds(pl.multiple_of(g * part, part), part), :]
        return remote(at, at, ag_s.at[b, s - 1, way], ag_r.at[b, s - 1, way], neighbour(way))

    def ag_conditions(s):
        return ((z >= s - 1) & (z <= groups - 2), (z <= groups - s) & (z >= 1))

    def ag_step(b, s):
        go = ag_conditions(s)
        for way in range(2):
            g = (z - s + 1, z + s - 1)[way]

            @pl.when(go[way])
            def _():
                if s > 1:
                    ag_copy(b, s - 1, way, g).wait_recv()
                ag_copy(b, s, way, g).start()

    def ag_finish(b):
        @pl.when(z == groups - 1)
        def _():
            for s in range(1, groups):
                ag_copy(b, s, 0, z - s).wait_recv()

        @pl.when(z == 0)
        def _():
            for s in range(1, groups):
                ag_copy(b, s, 1, z + s).wait_recv()

    def ag_drain(b):
        for s in range(1, groups):
            go = ag_conditions(s)
            for way in range(2):
                g = (z - s + 1, z + s - 1)[way]
                pl.when(go[way])(lambda: ag_copy(b, s, way, g).wait_send())

    def rs_copy(b, t, way, d):
        land = (from_left, from_right)[way]
        return remote(
            own.at[b % OWN_SLOTS, d],
            land.at[b, t - 1],
            rs_s.at[b, t - 1, way],
            rs_r.at[b, t - 1, way],
            neighbour(way),
        )

    rows_add = min(32, BC)

    def rs_load(b, t, way):
        return local((from_left, from_right)[way].at[b, t - 1], ld.at[way], loc.at[4 + way])

    def add_in(b, d, way):
        slot = b % OWN_SLOTS

        def body(i, carry):
            at = pl.ds(pl.multiple_of(i * rows_add, rows_add), rows_add)
            total = own[slot, d, at, :].astype(F32) + ld[way, at, :].astype(F32)
            own[slot, d, at, :] = total.astype(BF)
            return carry

        lax.fori_loop(0, BC // rows_add, body, 0)

    def rs_conditions(t):
        return (z <= t - 1, z >= groups - t)

    def rs_step(b, t):
        go = rs_conditions(t)
        ends = (z == 0, z == groups - 1)
        dest = (z + groups - t, z - groups + t)
        for way in range(2):
            d = dest[way]
            if t > 1:

                @pl.when(go[way] & jnp.logical_not(ends[way]))
                def _():
                    rs_copy(b, t - 1, way, d).wait_recv()
                    rs_load(b, t - 1, way).start()

        for way in range(2):
            d = dest[way]
            if t > 1:

                @pl.when(go[way] & jnp.logical_not(ends[way]))
                def _():
                    rs_load(b, t - 1, way).wait()
                    add_in(b, d, way)

            @pl.when(go[way])
            def _():
                rs_copy(b, t, way, d).start()

    def rs_drain(b):
        for t in range(1, groups):
            go = rs_conditions(t)
            for way in range(2):
                d = (z + groups - t, z - groups + t)[way]
                pl.when(go[way])(lambda: rs_copy(b, t, way, d).wait_send())

    def results(b, half):
        if b == 2:
            return ((g_query, g_key)[half], HD, 0, True)
        if b == 3:
            return ((g_value, g_dense)[half], HD, 0, half == 0)
        return ((g_up, g_down)[half], hidden, feed_of[b] * HD, half == 0)

    def bk_copy(b, k, half):
        array, size, offset, turned = results(b, half)
        at = pl.ds(pl.multiple_of(rank * size + offset, LANES), HD)
        if turned:
            rows = pl.ds(pl.multiple_of(prank[k] * depth, depth), depth)
            src, dst = fin_t.at[b % 2, half, rows, :], array.at[:, at]
        else:
            src, dst = fin.at[b % 2], array.at[at, :]
            if back != part:
                src = src.at[:, pl.ds(pl.multiple_of(prank[k] * depth, LANES), depth)]
        if k == 0:
            return local(src, dst, bk_l.at[b % 2, half])
        return remote(src, dst, bk_s.at[b % 2, k - 1, half], bk_r.at[b], peer[k])

    def bk_arrived(b):
        lanes = sum(depth if results(b, half)[3] else back for half in range(2))
        rows = w_all.at[b, pl.ds(0, (TP - 1) * lanes * HD // BC), :]
        local(rows, rows, bk_r.at[b]).wait()

    def bk_drain(b):
        for half in range(2):
            bk_copy(b, 0, half).wait()
            for k in range(1, TP):
                bk_copy(b, k, half).wait_send()

    def rs_finish(b):
        last = groups - 1
        inner = (z > 0, z < groups - 1)
        for way in range(2):

            @pl.when(inner[way])
            def _():
                rs_copy(b, last, way, z).wait_recv()
                rs_load(b, last, way).start()

        if b >= 2:
            bk_drain(b - 2)
        for way in range(2):
            pl.when(inner[way])(lambda: rs_load(b, last, way).wait())

        slot = b % OWN_SLOTS
        for half in range(2):
            turned = results(b, half)[3]

            def body(i, carry):
                unit = pl.multiple_of(i * LANES, LANES)
                at = pl.ds(half * HD + unit, LANES)
                total = own[slot, z, at, :].astype(F32)
                for way in range(2):
                    total += jnp.where(inner[way], ld[way, at, :].astype(F32), 0.0)
                if turned:
                    fin_t[b % 2, half, :, pl.ds(unit, LANES)] = total.T.astype(BF)
                else:
                    fin[b % 2, pl.ds(unit, LANES), :] = total.astype(BF)
                return carry

            lax.fori_loop(0, HD // LANES, body, 0)
        for k in (2, 3, 1, 0):
            for half in range(2):
                bk_copy(b, k, half).start()

    slot_qk, slot_vd = 2, 0
    slot_of = {0: 0, 1: 1, 2: slot_qk, 3: slot_vd, 4: 1, 5: 1}

    def w_load(b):
        return local(w_all.at[b], wv.at[slot_of[b]], loc.at[6 + slot_of[b]])

    def feed_forward(b):
        i = feed_of[b]
        slot = slot_of[b]
        lanes = slice(i * HD, (i + 1) * HD)

        def body(n, carry):
            at = pl.ds(pl.multiple_of(n * length, length), length)
            pre = dot_nn(big[1, at, :], wv[slot, :, :HD]) + bias[0:1, (3 + i) * HD : (4 + i) * HD]
            grad_act = dot_nn(big[2, at, :], wv[slot, :, HD:])
            cdf = 0.5 * (1.0 + lax.erf(pre * 0.7071067811865476))
            pdf = jnp.exp(-0.5 * pre * pre) * 0.3989422804014327
            act_v[0, at, lanes] = (pre * cdf).astype(BF)
            grad_pre = (grad_act * (cdf + pre * pdf)).astype(BF)
            act_v[1, at, lanes] = grad_pre
            return carry + jnp.sum(grad_pre.astype(F32), axis=0, keepdims=True)

        total = lax.fori_loop(0, TP, body, jnp.zeros((1, HD), F32))
        sv[0, pl.ds(8 + rank, 1), (3 + i) * HD : (4 + i) * HD] = total

    def feed_backward(b):
        slot = b % OWN_SLOTS
        i = feed_of[b]
        lanes = slice(i * HD, (i + 1) * HD)

        def body(d, carry):
            cols = pl.ds(pl.multiple_of(d * part, part), part)
            own[slot, d, :HD, :] = dot_tn(act_v[1, :, lanes], big[1, :, cols]).astype(BF)
            own[slot, d, HD:, :] = dot_tn(act_v[0, :, lanes], big[2, :, cols]).astype(BF)
            return carry

        lax.fori_loop(0, groups, body, 0)

    def attention(between):
        def body(n, carry):
            at = pl.ds(pl.multiple_of(n * length, length), length)
            grads = attend(
                big[0, at, :],
                big[2, at, :],
                wv.at[slot_qk],
                wv.at[slot_vd],
                bias[0:1, : 3 * HD],
                table[at, :],
            )
            for j, g in enumerate(grads):
                ga_v[at, j * HD : (j + 1) * HD] = g
            sums = [jnp.sum(g.astype(F32), axis=0, keepdims=True) for g in grads[:3]]
            carry = carry + jnp.concatenate(sums, axis=1)
            for j, some in enumerate(between):
                if some:

                    @pl.when(n == j)
                    def _():
                        for step in some:
                            run(step)

            return carry

        total = lax.fori_loop(0, TP, body, jnp.zeros((1, 3 * HD), F32))
        sv[0, pl.ds(8 + rank, 1), : 3 * HD] = total

    def attention_back(b):
        slot = b % OWN_SLOTS

        def body(d, carry):
            cols = pl.ds(pl.multiple_of(d * part, part), part)
            if b == 2:
                own[slot, d, :HD, :] = dot_tn(ga_v[:, :HD], big[0, :, cols]).astype(BF)
                own[slot, d, HD:, :] = dot_tn(ga_v[:, HD:BC], big[0, :, cols]).astype(BF)
            else:
                own[slot, d, :HD, :] = dot_tn(ga_v[:, BC : 3 * HD], big[0, :, cols]).astype(BF)
                own[slot, d, HD:, :] = dot_tn(ga_v[:, 3 * HD :], big[2, :, cols]).astype(BF)
            return carry

        lax.fori_loop(0, groups, body, 0)

    def bias_sum():
        rows = min(64, length)

        def body(i, carry):
            at = pl.ds(pl.multiple_of(i * rows, rows), rows)
            return carry + jnp.sum(big[2, at, :].astype(F32), axis=0, keepdims=True)

        total = lax.fori_loop(0, length // rows, body, jnp.zeros((1, width), F32))
        sv[0, 4:5, :] = total * 0.5

    def close_weights(b, half):
        i = feed_of[b]
        lanes = pl.ds((feeds if half == 0 else 0) * HD + i * HD, HD)
        return local(
            w_all.at[b, :, pl.ds(half * HD, HD)], big.at[0, :, lanes], loc.at[9 + 2 * i + half]
        )

    def close_load(b):
        for half in range(2):
            close_weights(b, half).start()

    def close_ready(half):
        for b in feed_of:
            close_weights(b, half).wait()

    sub = TILE // 2

    def staged(q, k, row, count):
        if q == 0 and k == 2:
            return stage.at[pl.ds(pl.multiple_of(row, count), count), :]
        return big.at[1 + q, pl.ds(pl.multiple_of(k * length + row, count), count), :]

    span = min(BC, width)

    def staged_part(q, k, h, i):
        if q == 0 and k == 3:
            rows = pl.ds(pl.multiple_of(i * length + h * TILE, TILE), TILE)
            return wv.at[slot_of[blocks - 1], rows, pl.ds(0, span)]
        cols = pl.ds(pl.multiple_of(i * span, span), span)
        return staged(q, k, h * TILE, TILE).at[:, cols]

    def close_copy(q, k, h, i):
        rows = pl.ds(pl.multiple_of(h * TILE, TILE), TILE)
        return remote(
            staged_part(q, k, h, i),
            core_in.at[q, k // 2, rows, pl.ds(i * span, span)],
            cl_s.at[q, k // 2, h],
            cl_r.at[q, k // 2, h],
            peer[1],
        )

    def close_tile(q, k, h, sem):
        rows = pl.ds(pl.multiple_of(h * TILE, TILE), TILE)
        at = core_in.at[q, k // 2, rows, :]
        return local(at, at, sem.at[q, k // 2, h])

    spans = range(width // span)

    def cross_copy(q, h, c):
        rows = pl.ds(pl.multiple_of(h * TILE + c * sub, sub), sub)
        return remote(
            staged(q, 2, h * TILE + c * sub, sub),
            cross_in.at[q, rows, :],
            cr_s.at[q, h, c],
            cr_r.at[q, h, c],
            peer[2],
        )

    def tensor_copy(q, h, c):
        rows = pl.ds(pl.multiple_of(h * TILE + c * sub, sub), sub)
        return remote(
            staged(q, 0, h * TILE + c * sub, sub),
            other_out.at[q, rows, :],
            ty_s.at[q, h, c],
            ty_r.at[q, h, c],
            dp,
            tensor=1 - ty,
        )

    def keep_copy(q, h, c):
        rows = pl.ds(pl.multiple_of(h * TILE + c * sub, sub), sub)
        return local(staged(q, 0, h * TILE + c * sub, sub), mine_out.at[q, rows, :], ke_s.at[q, h, c])

    def merge(q, h, c):
        cross_copy(q, h, c).wait_recv()
        rows = pl.ds(h * TILE + c * sub, sub)
        copy = local(cross_in.at[q, rows, :], xs.at[1, pl.ds(0, sub), :], loc.at[1])
        copy.start()
        copy.wait()
        rows_here = min(32, sub)
        mine = staged(q, 0, h * TILE + c * sub, sub)

        def body(i, carry):
            at = pl.ds(pl.multiple_of(i * rows_here, rows_here), rows_here)
            mine[at, :] = (mine[at, :].astype(F32) + xs[1, at, :].astype(F32)).astype(BF)
            return carry

        lax.fori_loop(0, sub // rows_here, body, 0)
        tensor_copy(q, h, c).start()
        keep_copy(q, h, c).start()

    ready = []

    def close(q, k):
        if q not in ready:
            ready.append(q)
            close_ready(1 - q)
            if q == 1:
                tok_sent(1)
        col = lambda v: jnp.sum(v, axis=0, keepdims=True)

        def tile(h, carry):
            at = pl.ds(pl.multiple_of(k * length + h * TILE, TILE), TILE)
            if q == 1:
                x_load(k, h, 0).start()
            if k in (0, 2):
                close_tile(q, k + 1, h, cl_r).wait()
                rows = pl.ds(pl.multiple_of(h * TILE, TILE), TILE)
                copy = local(core_in.at[q, k // 2, rows, :], xs.at[1], loc.at[1])
                copy.start()
            if q == 1:
                x_load(k, h, 0).wait()
                x = xs[0].astype(F32)
                mean = jnp.mean(x, axis=-1, keepdims=True)
                inverse = lax.rsqrt(jnp.mean(jnp.square(x - mean), axis=-1, keepdims=True) + 1e-05)
            if k in (0, 2):
                copy.wait()

            def body(i, carry):
                cols = pl.ds(pl.multiple_of(i * span, span), span)
                if q == 0:
                    total = dot_nt(act_v[0, at, :], big[0, cols, : feeds * HD])
                    total += dot_nt(ga_v[at, 3 * HD :], wv[slot_vd, cols, HD:])
                else:
                    hat = (xs[0, :, cols].astype(F32) - mean) * inverse
                    grad_f = dot_nt(act_v[1, at, :], big[0, cols, feeds * HD :])
                    sv[0, 2:3, cols] += col(grad_f * hat)
                    sv[0, 3:4, cols] += col(grad_f)
                    grad_a = dot_nt(ga_v[at, :BC], wv[slot_qk, cols, :])
                    grad_a += dot_nt(ga_v[at, BC : 3 * HD], wv[slot_vd, cols, :HD])
                    sv[0, 0:1, cols] += col(grad_a * hat)
                    sv[0, 1:2, cols] += col(grad_a)
                    total = grad_f * norms[2:3, cols] + grad_a * norms[0:1, cols]
                if k in (0, 2):
                    total += xs[1, :, cols].astype(F32)
                staged_part(q, k, h, i)[...] = total.astype(BF)
                return carry

            lax.fori_loop(0, width // span, body, 0)
            if k in (1, 3):
                for i in spans:
                    close_copy(q, k, h, i).start()
            if k == 2:
                for c in range(2):
                    cross_copy(q, h, c).start()
            return carry

        lax.fori_loop(0, length // TILE, tile, 0)

    def sv_copy(n):
        if n < rounds:
            return remote(
                sv.at[n], sv_in.at[n], sv_s.at[n], sv_r.at[n], lax.bitwise_xor(dp, 1 << n)
            )
        rows = pl.ds(0, 8)
        return remote(
            sv.at[n, rows], sv_in.at[n, rows], sv_s.at[n], sv_r.at[n], dp, tensor=1 - ty
        )

    def sv_step(n):
        if n > 0:
            sv_copy(n - 1).wait_recv()
        if n <= rounds:
            if n > 0:
                sv[n] = sv[n - 1] + sv_in[n - 1]
            sv_copy(n).start()
        else:
            sums_out[0:8] = sv[rounds, 0:8] + sv_in[rounds, 0:8]
            sums_out[8:16] = sv[rounds, 8:16]

    barrier = pltpu.get_barrier_semaphore()

    def greet(target, tensor):
        pl.semaphore_signal(barrier, inc=1, device_id=(target, tensor), device_id_type=MESH)

    greet(dp, 1 - ty)
    for k in range(1, TP):
        greet(peer[k], ty)
    bit = TP
    while bit < dp_size:
        greet(lax.bitwise_xor(dp, bit), ty)
        bit *= 2
    odd = lax.rem(z, 2) == 1
    up_more, down_more = odd & (z < groups - 1), jnp.logical_not(odd) & (z > 0)
    pl.when(up_more)(lambda: greet(neighbour(0), ty))
    pl.when(down_more)(lambda: greet(neighbour(1), ty))
    count = rounds + 2
    more = up_more | down_more
    pl.when(more)(lambda: pl.semaphore_wait(barrier, count + 1))
    pl.when(jnp.logical_not(more))(lambda: pl.semaphore_wait(barrier, count))

    steps = {
        A2A_START: a2a_start,
        A2A_WAIT: a2a_wait,
        TOK_START: tok_start,
        TOK_Y: tok_y,
        TOK_CORE: tok_core,
        TOK_WAIT: tok_wait,
        TAB_MAKE: tab_make,
        TAB_START: tab_start,
        TAB_CORE: tab_core,
        TAB_WAIT: tab_wait,
        PK: pk,
        PK_NORM: pk_norm,
        PK_BIAS: pk_bias,
        NORM: norm_slot,
        AG: ag_step,
        AG_FINISH: ag_finish,
        LOAD: lambda b: w_load(b).start(),
        LOAD_WAIT: lambda b: w_load(b).wait(),
        FF_FWD: feed_forward,
        FF_BWD: feed_backward,
        ATTN_BWD: attention_back,
        BIAS_SUM: bias_sum,
        RS: rs_step,
        RS_FINISH: rs_finish,
        RS_DRAIN: rs_drain,
        CLOSE_LOAD: close_load,
        CLOSE: close,
        MERGE: merge,
        SV: sv_step,
    }

    def run(step):
        steps[step[0]](*step[1:])

    sv[0] = jnp.zeros(sv.shape[1:], F32)
    ld[...] = jnp.zeros(ld.shape, BF)
    plan = make_schedule(groups)
    plan.insert(0, (TAB_MAKE,))
    rows_at = [plan.index((ATTN_ROW, n)) for n in range(TP)]
    for step in plan[: rows_at[0]]:
        run(step)
    attention([plan[i + 1 : j] for i, j in zip(rows_at, rows_at[1:])] + [[]])
    for step in plan[rows_at[-1] + 1 :]:
        run(step)

    drained = [step[1] for step in plan if step[0] == RS_DRAIN]
    for b in range(blocks):
        a2a_sent(b)
        ag_drain(b)
        if b not in drained:
            rs_drain(b)
    tok_own(0).wait()
    for which in range(2):
        tok_beside(which).wait_send()
        for c in range(2):
            tok_cross(which, c).wait_send()
    tok_sent(0)
    for hop in (1, 2, 3):
        tab_copy(hop).wait_send()
    for n in range(rounds):
        pk_copy(n).wait_send()
    for n in range(rounds + 1):
        sv_copy(n).wait_send()
    for q in range(2):
        for h in range(length // TILE):
            for k in (1, 3):
                close_tile(q, k, h, cl_s).wait()
            for c in range(2):
                cross_copy(q, h, c).wait_send()
                tensor_copy(q, h, c).wait_send()
                tensor_copy(q, h, c).wait_recv()
                keep_copy(q, h, c).wait()
    bk_drain(blocks - 2)
    bk_drain(blocks - 1)
    for b in range(blocks):
        bk_arrived(b)


def run_main(groups, x, cot, weights, segments, pack, bias_cols):
    length, width = x.shape
    depth = weights[0].shape[0]
    part = width // groups
    tokens = TP * length
    hidden = weights[4].shape[1] // TP
    feeds = hidden // HD
    blocks = feeds + 2
    dp_size = groups * TP
    rounds = dp_size.bit_length() - 1
    back = depth if depth % LANES == 0 else part
    cfg = (groups, part, depth, width, tokens, length, feeds, back, hidden, bias_cols)
    hbm = pl.BlockSpec(memory_space=pltpu.HBM)
    vmem = pl.BlockSpec(memory_space=pltpu.VMEM)
    sem = pltpu.SemaphoreType.DMA
    shape = jax.ShapeDtypeStruct
    tiles = length // TILE
    steps_in = (jnp.arange(LANES) % (ROT // 2)).astype(F32)
    freq = (10000.0 ** (-2.0 * steps_in / ROT)).reshape(1, LANES)
    return pl.pallas_call(
        functools.partial(main_kernel, cfg),
        out_shape=(
            shape((TP, length, width), BF),
            shape((blocks, width, BC), BF),
            shape((depth, TP * HD), BF),
            shape((depth, TP * HD), BF),
            shape((depth, TP * HD), BF),
            shape((TP * HD, back), BF),
            shape((depth, TP * hidden), BF),
            shape((TP * hidden, back), BF),
            shape((dp_size,) + pack.shape, F32),
            shape((2, length, width), BF),
            shape((2, length, width), BF),
            shape((16, width), F32),
            shape((blocks, groups, BC, part), BF),
            shape((blocks, groups, BC, part), BF),
            shape((2, 2, length, width), BF),
            shape((2, length, width), BF),
        ),
        in_specs=[hbm] * 8 + [vmem] * 2 + [hbm],
        out_specs=(hbm,) * 8 + (vmem,) + (hbm,) * 2 + (vmem,) + (hbm,) * 4,
        scratch_shapes=[
            pltpu.VMEM((3, tokens, width), BF),
            pltpu.VMEM((W_SLOTS, width, BC), BF),
            pltpu.VMEM((OWN_SLOTS, groups, BC, part), BF),
            pltpu.VMEM((2, HD, part), BF),
            pltpu.VMEM((2, 2, part, HD), BF),
            pltpu.VMEM((2, BC, part), BF),
            pltpu.VMEM((2, TILE, width), BF),
            pltpu.VMEM((2, tokens, feeds * HD), BF),
            pltpu.VMEM((tokens, 4 * HD), BF),
            pltpu.VMEM((tokens, LANES), F32),
            pltpu.VMEM((8, width), F32),
            pltpu.VMEM((8, (3 + feeds) * HD), F32),
            pltpu.VMEM((rounds + 1, 16, width), F32),
            pltpu.VMEM((rounds + 1, 16, width), F32),
            sem((blocks,)),
            sem((blocks,)),
            sem((3, 7)),
            sem((3, 7)),
            sem((blocks, groups - 1, 2)),
            sem((blocks, groups - 1, 2)),
            sem((blocks, groups - 1, 2)),
            sem((blocks, groups - 1, 2)),
            sem((2, TP - 1, 2)),
            sem((blocks,)),
            sem((2, 2)),
            sem((rounds,)),
            sem((rounds,)),
            sem((rounds + 1,)),
            sem((rounds + 1,)),
            sem((2, 2, tiles)),
            sem((2, 2, tiles)),
            sem((2, tiles, 2)),
            sem((2, tiles, 2)),
            sem((2, tiles, 2)),
            sem((2, tiles, 2)),
            sem((2, tiles, 2)),
            sem((9 + 2 * feeds,)),
            pltpu.VMEM((length, width), BF),
        ],
        compiler_params=pltpu.CompilerParams(
            collective_id=0, has_side_effects=True, vmem_limit_bytes=67043328
        ),
        name="main",
    )(x, cot, *weights, segments, freq, pack)


def prepare_kernel(dense, down, *refs):
    small, (dense_t, down_t, pack) = refs[:10], refs[10:]
    dense_t[...] = dense[...].astype(F32).T.astype(BF)
    down_t[...] = down[...].astype(F32).T.astype(BF)

    @pl.when(pl.program_id(0) == 0)
    def _():
        pack[...] = jnp.zeros(pack.shape, F32)
        row = 0
        for i, ref in enumerate(small):
            value = ref[...].astype(F32)
            if value.ndim == 1:
                value = value.reshape(1, -1)
            elif row == 6:
                row = 8
            rows, lanes = value.shape
            pack[row : row + rows, 0:lanes] = value
            row += rows


def prepare(dense, down, small):
    steps = 4
    depth = dense.shape[1]
    rows = 8 + sum(a.shape[0] for a in small[6:])
    tile = lambda a: pl.BlockSpec((a.shape[0] // steps, depth), lambda i: (i, 0))
    turned = lambda a: pl.BlockSpec((depth, a.shape[0] // steps), lambda i: (0, i))
    shape = jax.ShapeDtypeStruct
    packed = (rows + -rows % 8, LANES)
    return pl.pallas_call(
        prepare_kernel,
        grid=(steps,),
        out_shape=(
            shape(dense.shape[::-1], BF),
            shape(down.shape[::-1], BF),
            shape(packed, F32),
        ),
        in_specs=[tile(dense), tile(down)]
        + [pl.BlockSpec(a.shape, lambda i, n=a.ndim: (0,) * n) for a in small],
        out_specs=[turned(dense), turned(down), pl.BlockSpec(packed, lambda i: (0, 0))],
        compiler_params=pltpu.CompilerParams(vmem_limit_bytes=67043328),
        name="prepare",
    )(dense, down, *small)


def finish_kernel(cols, mine, other, x_ref, cot, packs, sums, *refs):
    grads, (hidden, grad_in), made, small, bias = refs[:6], refs[6:8], refs[8:14], refs[14:-1], refs[-1]
    devices = packs.shape[0]
    depth = bias.shape[1] // devices

    @pl.when(pl.program_id(0) == 0)
    def _():
        for j in range(devices):
            bias[0:1, j * depth : (j + 1) * depth] = packs[j, 4:5, :depth] + packs[j, 5:6, :depth]
        dp = lax.axis_index("dp")
        out_query, out_key, out_value, out_up = small[:4]

        def mine_of(lanes):
            wide = pltpu.roll(sums[8 : 8 + 8, lanes], lax.rem(HD - dp * cols, HD), 1)
            return wide[:TP, :cols]

        out_query[...] = mine_of(slice(0, HD))
        out_key[...] = sums[8 : 8 + TP, HD : HD + ROT]
        out_value[...] = mine_of(slice(2 * HD, 3 * HD))
        units = out_up.shape[0] // TP
        for i in range(units):
            piece = mine_of(slice((3 + i) * HD, (4 + i) * HD))
            for rank in range(TP):
                row = rank * units + i
                out_up[row : row + 1, :] = piece[rank : rank + 1, :]
        lanes = slice(0, depth * devices)
        if depth % LANES == 0:
            lanes = pl.ds(pl.multiple_of(dp * depth, LANES), depth)
        for row, out in zip((0, 1, 2, 3, 4, 4), small[4:]):
            out[...] = sums[row : row + 1, lanes].reshape(out.shape)

    x = x_ref[...].astype(F32)
    hidden[...] = (x + (mine[0].astype(F32) + other[0].astype(F32)) + bias[...]).astype(BF)
    hat, inverse = normed_hat(x)
    h = mine[1].astype(F32) + other[1].astype(F32)
    grad_in[...] = cot[...].astype(F32) + inverse * (
        h
        - jnp.mean(h, axis=-1, keepdims=True)
        - hat * jnp.mean(h * hat, axis=-1, keepdims=True)
    )
    for source, target in zip(grads, made):
        target[...] = source[...].astype(F32)


def finish(mine, other, x, cot, packs, sums, grads, cols):
    length, width = x.shape
    depth = grads[0].shape[0]
    steps = max(1, min(4, depth // 16))
    tile = lambda a: pl.BlockSpec((a.shape[0] // steps, a.shape[1]), lambda i: (i, 0))
    pair = pl.BlockSpec((2, length // steps, width), lambda i: (0, i, 0))
    shape = jax.ShapeDtypeStruct
    units = grads[4].shape[1] // HD
    whole = lambda s: pl.BlockSpec(s, lambda i: (0,) * len(s))
    small = [(TP, cols), (TP, ROT), (TP, cols), (units, cols)]
    small += [(depth if depth % LANES == 0 else width,)] * 6
    return pl.pallas_call(
        functools.partial(finish_kernel, cols),
        grid=(steps,),
        out_shape=(shape(x.shape, BF), shape(x.shape, F32))
        + tuple(shape(g.shape, F32) for g in grads)
        + tuple(shape(s, F32) for s in small),
        in_specs=[pair, pair, tile(x), tile(cot), whole(packs.shape), whole(sums.shape)]
        + [tile(g) for g in grads],
        out_specs=[tile(x), tile(x)] + [tile(g) for g in grads] + [whole(s) for s in small],
        scratch_shapes=[pltpu.VMEM((1, width), F32)],
        compiler_params=pltpu.CompilerParams(vmem_limit_bytes=67043328),
        name="finish",
    )(mine, other, x, cot, packs, sums, *grads)


def make_shards(dp_size):
    groups = dp_size // TP

    def shards(
        hidden_in,
        segments,
        cotangent,
        w_query,
        w_key,
        w_value,
        w_dense,
        w_up,
        w_down,
        bias_query,
        bias_key,
        bias_value,
        bias_dense,
        bias_up,
        bias_down,
        attend_gain,
        attend_shift,
        feed_gain,
        feed_shift,
    ):
        dp = lax.axis_index("dp")
        rank = dp % TP
        length, width = hidden_in.shape
        depth = w_query.shape[0]
        cols = bias_query.shape[1]

        small = (attend_gain, attend_shift, feed_gain, feed_shift, bias_dense, bias_down)
        small += (bias_query, bias_key, bias_value, bias_up)
        dense_t, down_t, pack = prepare(w_dense, w_down, small)
        weights = (w_query, w_key, w_value, dense_t, w_up, down_t)
        made = run_main(groups, hidden_in, cotangent, weights, segments, pack, cols)
        grads, (packs, mine, other, sums) = made[2:8], made[8:12]

        if grads[3].shape[1] != depth:
            mine_of = lambda g: lax.dynamic_slice_in_dim(g, rank * depth, depth, 1)
            grads = grads[:3] + (mine_of(grads[3]), grads[4], mine_of(grads[5]))
        done = finish(mine, other, hidden_in, cotangent, packs, sums, grads, cols)
        out_query, out_key, out_value, out_up = done[8:12]
        vec = done[12:]
        if vec[0].shape[0] != depth:
            vec = [lax.dynamic_slice_in_dim(v, dp * depth, depth, 0) for v in vec]
        return done[:8] + (
            out_query,
            out_key,
            out_value,
            vec[4],
            out_up,
            vec[5],
            vec[0],
            vec[1],
            vec[2],
            vec[3],
        )

    return shards


def solution(mesh):
    shards = make_shards(mesh.shape["dp"])
    in_specs = (
        P("dp", None),
        P("dp", None),
        P("dp", None),
        P("dp", "tensor"),
        P("dp", "tensor"),
        P("dp", "tensor"),
        P("tensor", "dp"),
        P("dp", "tensor"),
        P("tensor", "dp"),
        P("tensor", "dp"),
        P("tensor", "dp"),
        P("tensor", "dp"),
        P("dp"),
        P("tensor", "dp"),
        P("dp"),
        P("dp"),
        P("dp"),
        P("dp"),
        P("dp"),
    )
    out_specs = (
        P("dp", None),
        P("dp", None),
        P("dp", "tensor"),
        P("dp", "tensor"),
        P("dp", "tensor"),
        P("tensor", "dp"),
        P("dp", "tensor"),
        P("tensor", "dp"),
        P("tensor", "dp"),
        P("tensor", None),
        P("tensor", "dp"),
        P("dp"),
        P("tensor", "dp"),
        P("dp"),
        P("dp"),
        P("dp"),
        P("dp"),
        P("dp"),
    )
    return jax.shard_map(shards, mesh=mesh, in_specs=in_specs, out_specs=out_specs, check_vma=False)
```
